512 devices in a mesh: outer: 16 (over x, y_lo), inner: 32 (over z, y_hi, core).
Axes of the slice: x: 4, y: 8 (y_hi: 2, y_lo: 4; y = y_hi * 4 + y_lo), z: 8, core: 2. Of those that a mesh axis runs over, the one named last changes fastest.
Arguments:
- queries: bfloat16 [131072, 512], P(('outer', 'inner')), may hold values from -56 to 56
- keys: bfloat16 [131072, 512], P(('outer', 'inner')), may hold values from -48 to 48
- values: bfloat16 [131072, 512], P(('outer', 'inner')), may hold values from -6 to 6
- out_weight: bfloat16 [512, 768], replicated, may hold values from -0.25 to 0.25
- slide_lengths: int32 [16], replicated, may hold values from 1 to 98304, 131072 in all
Outputs:
- mixed_output: bfloat16 [131072, 768], P(('outer', 'inner'))
The draws below stay inside these ranges and needn't reach their ends.
Inputs may be any that keep to these rules, and one draw needn't show every extreme that they name: `slide_lengths`: the lengths sum to 131072.
All inputs are finite; a program needn't handle non-finite values.
Results may differ from the reference program's by a relative error of at most 0.0052.
Values may be sent and summed in bfloat16 or wider, within the bound.
A program may use at most 64 MiB of HBM per device.

```python
import math
import jax
import jax.numpy as jnp
import numpy as np
from jax import lax

D = 768
HEADS = 8
HEAD_DIM = 64
SPARSE = 1024
SLIDES = 16
HD = 512
TOKENS = 131072
MID_RATE = 8
TOP_RATE = 128


def draw_pair(key):
    seeds = jax.random.split(jax.random.fold_in(key, 4242), 2)
    width = HEADS * HEAD_DIM
    query_matrix = 3.0 * jax.random.truncated_normal(seeds[0], -6.0, 6.0, (TOKENS, width), jnp.float32)
    keys_matrix = jax.random.truncated_normal(seeds[1], -6.0, 6.0, (TOKENS, width), jnp.float32)
    return (query_matrix, keys_matrix)


def draw_queries(key, part):
    return draw_pair(key)[0].astype(jnp.bfloat16)


def draw_keys(key, part):
    return draw_pair(key)[1].astype(jnp.bfloat16)


def block_levels(own_key, extent, cuts, low, top_value):
    factor_of = 1.0
    for position, parts in cuts:
        draws = jax.random.uniform(jax.random.fold_in(jax.random.fold_in(own_key, 6), position), (parts,), jnp.float32, low / len(cuts), top_value / len(cuts))
        factor_of = factor_of * jnp.repeat(jnp.exp(draws), extent[position] // parts).reshape((-1,) + (1,) * (len(extent) - 1 - position))
    return factor_of


def profile(count, total, reach, skew):
    loads = [(1 << 20) // math.isqrt(rank ** skew) + 1 for rank in range(2, count + 1)]
    surplus, holding = total - reach - (count - 1), [1] * (count - 1)
    while surplus > 0:
        movable = [i for i in range(count - 1) if holding[i] < reach]
        whole, remaining = sum([loads[i] for i in movable]), surplus
        for i in movable:
            addition = min(reach - holding[i], max(1, remaining * loads[i] // whole), surplus)
            holding[i] = holding[i] + addition
            surplus = surplus - addition
    return np.array([reach] + holding)


def ragged(own_key, number_of, total, limit, skew):
    if number_of == 2:
        one = jax.random.randint(own_key, (), max(1, total - limit), min(limit, total - 1) + 1)
        return jnp.stack([one, total - one])
    lengths = jnp.asarray(profile(number_of, total, limit, skew), jnp.int32)
    twos = (number_of - 1) // 2
    giver, receiver = lengths[1:1 + 2 * twos:2], lengths[2:2 + 2 * twos:2]
    slack = jnp.minimum(giver - 1, limit - receiver)
    moved = jax.random.randint(jax.random.fold_in(own_key, 1), (twos,), 0, 1 << 20) % (slack + 1)
    lengths = lengths.at[1:1 + 2 * twos:2].set(giver - moved).at[2:2 + 2 * twos:2].set(receiver + moved)
    return lengths[jax.random.permutation(jax.random.fold_in(own_key, 2), number_of)]


def scatter_about(own_key, dims, scale, bound, cuts=(), kind=jnp.bfloat16):
    drawn = scale * jax.random.normal(own_key, dims, jnp.float32)
    if cuts:
        drawn = drawn * block_levels(own_key, dims, cuts, -0.22, 0.18)
    return jnp.clip(drawn, -bound, bound).astype(kind)


def setup_inputs(seed: int = 0) -> dict:
    streams_of = jax.random.split(jax.random.key(seed), 6)
    queries = draw_queries(jax.random.fold_in(streams_of[5], 71), 0)
    keys = draw_keys(jax.random.fold_in(streams_of[5], 71), 0)
    values = scatter_about(streams_of[2], (TOKENS, HD), 1.0, 6.0, ((0, 512),))
    out_weight = scatter_about(streams_of[3], (HD, D), HD ** -0.5, 0.25)
    slide_lengths = ragged(streams_of[4], SLIDES, TOKENS, 3 * TOKENS // 4, 2).astype(jnp.int32)
    return dict(queries=queries, keys=keys, values=values, out_weight=out_weight, slide_lengths=slide_lengths)


masked_score = -1e30


def slide_index(positions, slide_ends):
    return jnp.sum((positions[:, None] >= slide_ends[None, :]).astype(jnp.int32), axis=1).astype(jnp.int32)


def segment_attention(query_rows, key_rows, value_rows, query_slides, key_slides):
    scores = jnp.dot(query_rows, key_rows.T, preferred_element_type=jnp.float32) * (HEAD_DIM ** -0.5)
    scores = jnp.where(query_slides[:, None] == key_slides[None, :], scores, masked_score)
    row_max = jnp.max(scores, axis=1, keepdims=True)
    expos = jnp.exp(scores - row_max)
    totals = jnp.sum(expos, axis=1, keepdims=True)
    probs = expos.astype(jnp.bfloat16)
    branch = jnp.dot(probs, value_rows, preferred_element_type=jnp.float32) / totals
    return branch, row_max[:, 0] + jnp.log(totals[:, 0])


def mix_levels(first, second, third):
    largest = jnp.maximum(jnp.maximum(first[1], second[1]), third[1])
    weighted = jnp.zeros_like(first[0])
    weight_sum = jnp.zeros_like(first[1])
    for branch, branch_lse in (first, second, third):
        factor = jnp.exp(branch_lse - largest)
        weighted = weighted + factor[:, None] * branch
        weight_sum = weight_sum + factor
    return weighted / weight_sum[:, None]


def level_branch(queries, keys, values, slides, step_rate, head_index):
    offset = head_index % step_rate
    first_column = head_index * HEAD_DIM

    def select_head(matrix):
        grouped = matrix[:, first_column:first_column + HEAD_DIM].reshape(TOKENS // step_rate, step_rate, HEAD_DIM)
        return grouped[:, offset, :].reshape(-1, SPARSE, HEAD_DIM)

    picked_slides = slides.reshape(TOKENS // step_rate, step_rate)[:, offset].reshape(-1, SPARSE)

    def one_segment(pieces):
        return segment_attention(pieces[0], pieces[1], pieces[2], pieces[3], pieces[3])

    branch, branch_lse = lax.map(one_segment, (select_head(queries), select_head(keys), select_head(values), picked_slides))
    full_branch = jnp.zeros((TOKENS // step_rate, step_rate, HEAD_DIM), jnp.float32)
    full_branch = full_branch.at[:, offset, :].set(branch.reshape(-1, HEAD_DIM)).reshape(TOKENS, HEAD_DIM)
    full_lse = jnp.full((TOKENS // step_rate, step_rate), masked_score, jnp.float32)
    full_lse = full_lse.at[:, offset].set(branch_lse.reshape(-1)).reshape(TOKENS)
    return full_branch, full_lse


def reference(queries, keys, values, out_weight, slide_lengths):
    slide_ends = jnp.cumsum(slide_lengths).astype(jnp.int32)
    slides = slide_index(jnp.arange(TOKENS, dtype=jnp.int32), slide_ends)
    head_outputs = []
    for head_index in range(HEADS):
        levels = [level_branch(queries, keys, values, slides, step_rate, head_index) for step_rate in (1, MID_RATE, TOP_RATE)]
        head_outputs.append(mix_levels(levels[0], levels[1], levels[2]))
    attention = jnp.concatenate(head_outputs, axis=1).astype(jnp.bfloat16)
    return jnp.dot(attention, out_weight, preferred_element_type=jnp.float32).astype(jnp.bfloat16)
```

```python
import jax
import jax.numpy as jnp
from jax import lax
from jax.experimental import pallas as pl
from jax.experimental.pallas import tpu as pltpu
from jax.sharding import PartitionSpec as P

HEADS = 8
HEAD_DIM = 64
SPARSE = 1024
SLIDES = 16
TOK = 256
ROWS = 32
MESH = pl.DeviceIdType.MESH
BF = jnp.bfloat16
F32 = jnp.float32

masked_score = -1e30


def iota(shape, dim):
    return lax.broadcasted_iota(jnp.int32, shape, dim)


def nt_dot(a, b):
    return lax.dot_general(a, b, (((1,), (1,)), ((), ())), preferred_element_type=F32)


def nn_dot(a, b):
    return lax.dot_general(a, b, (((1,), (0,)), ((), ())), preferred_element_type=F32)


def one_hot(mask):
    return jnp.where(mask, 1.0, 0.0).astype(BF)


def attend(q, parts, q_ids, k_ids):
    scores = jnp.concatenate([nt_dot(q, kv) for kv in parts], axis=1)
    scores = jnp.where(q_ids == k_ids, scores, masked_score)
    row_max = jnp.max(scores, axis=1, keepdims=True)
    expos = jnp.exp(scores - row_max)
    total = jnp.sum(expos, axis=1, keepdims=True)
    probs = expos.astype(BF)
    mixed, at = None, 0
    for kv in parts:
        term = nn_dot(probs[:, at : at + kv.shape[0]], kv)
        mixed = term if mixed is None else mixed + term
        at += kv.shape[0]
    return mixed / total, row_max + jnp.log(total)


def kernel(
    q_ref, k_ref, v_ref, w_ref, len_ref, out_ref,
    kv, qs, mkv, qmid, topkv, mid_out, top_out, mid_res, top_res, att, diag_o, diag_l,
    ids_q, ids_k,
    s_sib, r_sib, s_yd, r_yd, s_y, r_y, s_fw, r_fw, s_mz, r_mz, s_qz, r_qz,
    s_ty, r_ty, s_tx, r_tx, s_mr, r_mr, s_tr, r_tr,
):
    outer = lax.axis_index("outer")
    inner = lax.axis_index("inner")
    x, y_lo = outer // 4, outer % 4
    z, side, core = inner // 4, (inner // 2) % 2, inner % 2
    y = side * 4 + y_lo

    def at_z(zz, c):
        return (outer, zz * 4 + side * 2 + c)

    def at_xy(xx, yy):
        return (xx * 4 + yy % 4, z * 4 + (yy // 4) * 2 + core)

    def send(src, dst, s, r, device):
        return pltpu.make_async_remote_copy(
            src_ref=src, dst_ref=dst, send_sem=s, recv_sem=r, device_id=device, device_id_type=MESH
        )

    partner = (outer, z * 4 + (1 - side) * 2 + core)
    sibling = at_z(z, 1 - core)
    step2 = 2 - 4 * core
    y_to = [at_xy(x, (y + 1) % 8), at_xy(x, (y + 7) % 8), at_xy(x, (y + 8 + step2) % 8)]
    y_from = [y_to[0], y_to[1], at_xy(x, (y + 8 - step2) % 8)]
    x_to = [at_xy((x + 1) % 4, y), at_xy((x + 3) % 4, y), at_xy((x + 2) % 4, y)]
    z_to = [(z + k) % 8 for k in range(1, 8)]

    barrier = pltpu.get_barrier_semaphore()
    greet = [partner, sibling] + y_from + x_to
    for zz in z_to:
        greet += [at_z(zz, 0), at_z(zz, 1)]
    for device in greet:
        pl.semaphore_signal(barrier, inc=1, device_id=device, device_id_type=MESH)

    row, col = iota((TOK, TOK), 0), iota((TOK, TOK), 1)
    perm = one_hot(col == 8 * (row % ROWS) + row // ROWS)
    low = iota((TOK, 128), 1) < HEAD_DIM
    for p in range(4):
        lanes = slice(p * 128, (p + 1) * 128)
        keys = pltpu.roll(nn_dot(perm, k_ref[:, lanes]), 64, 1)
        vals = nn_dot(perm, v_ref[:, lanes])
        kv[0, 2 * p] = jnp.where(low, vals, keys).astype(BF).reshape(8, ROWS, 128)
        kv[0, 2 * p + 1] = jnp.where(low, keys, vals).astype(BF).reshape(8, ROWS, 128)
    for p in range(4):
        lanes = slice(p * 128, (p + 1) * 128)
        rows = pltpu.roll(nn_dot(perm, q_ref[:, lanes]), 64, 1) * HEAD_DIM**-0.5
        qs[2 * p] = jnp.where(low, 0.0, rows).astype(BF).reshape(8, ROWS, 128)
        qs[2 * p + 1] = jnp.where(low, rows, 0.0).astype(BF).reshape(8, ROWS, 128)

    pl.semaphore_wait(barrier, len(greet))

    slot_own = z * 4 + side * 2 + core
    slot_far = z * 4 + (1 - side) * 2 + core
    for h in range(HEADS):
        send(kv.at[0, h, h], kv.at[2, h, h], s_yd, r_yd, partner).start()
    for zz in z_to:
        for c in (core, 1 - core):
            send(kv.at[0, zz, zz], mkv.at[slot_own], s_mz, r_mz, at_z(zz, c)).start()
        send(qs.at[zz, zz], qmid.at[z], s_qz, r_qz, at_z(zz, core)).start()
    send(kv.at[0, z, z], mkv.at[slot_own], s_mz, r_mz, sibling).start()
    for h in range(HEADS):
        if h > 0:
            send(kv.at[0, h, 0:h], kv.at[2, h, 0:h], s_y.at[h], r_y.at[h], partner).start()
        if h < 7:
            send(kv.at[0, h, h + 1 : 8], kv.at[2, h, h + 1 : 8], s_y.at[h], r_y.at[h], partner).start()
    whole = send(kv.at[0], kv.at[1], s_sib, r_sib, sibling)
    whole.start()
    mkv[slot_own] = kv[0, z, z]
    qmid[z] = qs[z, z]

    ends, running = [], jnp.int32(0)
    for j in range(SLIDES):
        running = running + len_ref[j]
        ends.append(running)

    def slides(positions):
        found = jnp.zeros(positions.shape, jnp.int32)
        for end in ends:
            found = found + (positions >= end).astype(jnp.int32)
        return found

    block = outer * (32 * TOK)
    first = block + inner * TOK
    r = iota((TOK, 1), 0)
    ids_q[...] = jnp.broadcast_to(slides(first + 8 * (r % ROWS) + r // ROWS), (TOK, 128))
    n = iota((1, SPARSE), 1)
    slot, n = n // TOK, n % TOK
    far, other = slot // 2, slot % 2
    device = z * 4 + (side + far - 2 * far * side) * 2 + (core + other - 2 * other * core)
    ids_k[...] = jnp.broadcast_to(
        slides(block + device * TOK + 8 * (n % ROWS) + n // ROWS), (8, SPARSE)
    )

    send(kv.at[0, 0], kv.at[2, 0], s_yd, r_yd, partner).wait_recv()
    for zz in z_to:
        for c in (core, 1 - core):
            send(kv.at[2, zz, zz], mkv.at[slot_far], s_mz, r_mz, at_z(zz, c)).start()
    send(kv.at[2, z, z], mkv.at[slot_far], s_mz, r_mz, sibling).start()
    mkv[slot_far] = kv[2, z, z]
    all_mz = send(mkv.at[0:30], mkv.at[0:30], s_mz, r_mz, sibling)
    all_mz.wait_recv()
    all_qz = send(qmid.at[0:7], qmid.at[0:7], s_qz, r_qz, sibling)
    all_qz.wait_recv()

    mid_kv = mkv[...].reshape(SPARSE, 128)
    mid_q = qmid[...].reshape(TOK, 128)
    row, col = iota((64, SPARSE), 0), iota((64, SPARSE), 1)
    topkv[x, y_lo] = nn_dot(one_hot(col == 16 * row), mid_kv).astype(BF)
    row, col = iota((64, TOK), 0), iota((64, TOK), 1)
    pick = (row % 8 < 2) & (col == row // 8 * ROWS + row % 8 * 16)
    top_q = nn_dot(one_hot(pick), mid_q).astype(BF)
    for device in y_to:
        send(topkv.at[x, y_lo], topkv.at[x, y_lo], s_ty, r_ty, device).start()

    v_low = z % 2
    r, n = iota((TOK, 1), 0), iota((1, SPARSE), 1)
    mid_ids_q = slides(block + ((r // ROWS) * 4 + side * 2 + core) * TOK + 8 * (r % ROWS) + z)
    mid_ids_k = slides(block + (n // ROWS) * TOK + 8 * (n % ROWS) + z)
    branch, branch_lse = attend(mid_q, [mid_kv], mid_ids_q, mid_ids_k)
    holds = iota((TOK, 128), 1) // HEAD_DIM == v_low
    mid_out[...] = jnp.where(holds, branch, branch_lse).reshape(8, ROWS, 128)
    for zz in z_to:
        send(mid_out.at[zz], mid_res.at[z], s_mr, r_mr, at_z(zz, core)).start()
    mid_res[z] = mid_out[z]

    all_ty = send(topkv.at[0, 0:3], topkv.at[0, 0:3], s_ty, r_ty, sibling)
    all_ty.wait_recv()
    for device in x_to:
        send(topkv.at[x], topkv.at[x], s_tx, r_tx, device).start()

    whole.wait_recv()

    def pair(p, _):
        both, lses = [], []
        for e in range(2):
            h = 2 * p + e
            send(kv.at[0, h, 0:7], kv.at[2, h, 0:7], s_y.at[h], r_y.at[h], partner).wait_recv()
            forward = send(kv.at[2, h], kv.at[3, h], s_fw.at[h], r_fw.at[h], sibling)
            forward.start()
            forward.wait_recv()
            parts = [kv[s, h].reshape(TOK, 128) for s in range(4)]
            branch, branch_lse = attend(
                qs[h].reshape(TOK, 128), parts, ids_q[:, 0:1], ids_k[0:1, :]
            )
            diag_o[e] = branch
            diag_l[e] = jnp.broadcast_to(branch_lse, (TOK, 128))
            both.append(branch)
        att[p] = jnp.where(low, both[0], both[1]).astype(BF)
        for e in range(2):
            h = 2 * p + e
            start = pl.multiple_of(h * ROWS, ROWS)
            diag_o[2, pl.ds(start, ROWS)] = diag_o[e, pl.ds(start, ROWS)]
            diag_l[2, pl.ds(start, ROWS)] = diag_l[e, pl.ds(start, ROWS)]
        return _

    lax.fori_loop(0, 1, pair, 0)

    all_tx = send(topkv.at[0:3], topkv.at[0:3], s_tx, r_tx, sibling)
    all_tx.wait_recv()
    r, n = iota((64, 1), 0), iota((1, SPARSE), 1)
    top_ids_q = slides(block + ((r // 8) * 4 + side * 2 + core) * TOK + (r % 8) * 128 + z)
    top_ids_k = slides(n * 128 + z)
    branch, branch_lse = attend(top_q, [topkv[...].reshape(SPARSE, 128)], top_ids_q, top_ids_k)
    holds = iota((64, 128), 1) // HEAD_DIM == v_low
    top_out[...] = jnp.where(holds, branch, branch_lse).reshape(8, 8, 128)
    for zz in z_to:
        send(top_out.at[zz], top_res.at[z], s_tr, r_tr, at_z(zz, core)).start()
    top_res[z] = top_out[z]

    lax.fori_loop(1, 4, pair, 0)

    all_mr = send(mid_out.at[0:7], mid_res.at[0:7], s_mr, r_mr, sibling)
    all_mr.wait_recv()
    all_tr = send(top_out.at[0:7], top_res.at[0:7], s_tr, r_tr, sibling)
    all_tr.wait_recv()
    row = iota((ROWS, 1), 0)
    for h in range(HEADS):
        v_at = h % 2 * HEAD_DIM
        l_at = HEAD_DIM - v_at
        rows = slice(h * ROWS, (h + 1) * ROWS)
        mid, top = mid_res[h], top_res[h]
        top = jnp.where(row == 0, top[0:1], top[1:2])
        lse1 = diag_l[2, rows, 0:1]
        lse2 = mid[:, l_at : l_at + 1]
        lse3 = jnp.where(row % 16 == 0, top[:, l_at : l_at + 1], masked_score)
        largest = jnp.maximum(jnp.maximum(lse1, lse2), lse3)
        f1, f2, f3 = jnp.exp(lse1 - largest), jnp.exp(lse2 - largest), jnp.exp(lse3 - largest)
        mixed = (f1 * diag_o[2, rows] + f2 * mid + f3 * top) / (f1 + f2 + f3)
        att[h // 2, rows, v_at : v_at + HEAD_DIM] = mixed[:, v_at : v_at + HEAD_DIM].astype(BF)
    row, col = iota((TOK, TOK), 0), iota((TOK, TOK), 1)
    back = one_hot(row == 8 * (col % ROWS) + col // ROWS)
    total = None
    for p in range(4):
        rows = nn_dot(back, att[p]).astype(BF)
        term = nn_dot(rows, w_ref[p * 128 : (p + 1) * 128, :])
        total = term if total is None else total + term
    out_ref[...] = total.astype(BF)

    whole.wait_send()
    send(kv.at[0, 0], kv.at[2, 0], s_yd, r_yd, partner).wait_send()
    for h in range(HEADS):
        send(kv.at[0, h, 0:7], kv.at[2, h, 0:7], s_y.at[h], r_y.at[h], partner).wait_send()
        send(kv.at[2, h], kv.at[3, h], s_fw.at[h], r_fw.at[h], sibling).wait_send()
    all_mz.wait_send()
    all_qz.wait_send()
    all_ty.wait_send()
    all_tx.wait_send()
    all_mr.wait_send()
    all_tr.wait_send()


def shards(queries, keys, values, out_weight, slide_lengths):
    vmem = pl.BlockSpec(memory_space=pltpu.VMEM)
    dma = pltpu.SemaphoreType.DMA
    return pl.pallas_call(
        kernel,
        out_shape=jax.ShapeDtypeStruct((TOK, out_weight.shape[1]), BF),
        in_specs=[vmem] * 4 + [pl.BlockSpec(memory_space=pltpu.SMEM)],
        out_specs=vmem,
        scratch_shapes=[
            pltpu.VMEM((4, HEADS, 8, ROWS, 128), BF),
            pltpu.VMEM((HEADS, 8, ROWS, 128), BF),
            pltpu.VMEM((32, ROWS, 128), BF),
            pltpu.VMEM((8, ROWS, 128), BF),
            pltpu.VMEM((4, 4, 64, 128), BF),
            pltpu.VMEM((8, ROWS, 128), F32),
            pltpu.VMEM((8, 8, 128), F32),
            pltpu.VMEM((8, ROWS, 128), F32),
            pltpu.VMEM((8, 8, 128), F32),
            pltpu.VMEM((4, TOK, 128), BF),
            pltpu.VMEM((3, TOK, 128), F32),
            pltpu.VMEM((3, TOK, 128), F32),
            pltpu.VMEM((TOK, 128), jnp.int32),
            pltpu.VMEM((8, SPARSE), jnp.int32),
            dma, dma, dma, dma, dma((8,)), dma((8,)), dma((8,)), dma((8,)),
            dma, dma, dma, dma, dma, dma, dma, dma, dma, dma, dma, dma,
        ],
        compiler_params=pltpu.CompilerParams(
            collective_id=0, has_side_effects=True, vmem_limit_bytes=48 * 1024 * 1024
        ),
        name="dilated",
    )(queries, keys, values, out_weight, slide_lengths)


def solution(mesh):
    rows = P(("outer", "inner"), None)
    return jax.shard_map(
        shards, mesh=mesh, in_specs=(rows, rows, rows, P(), P()), out_specs=rows, check_vma=False
    )
```

```python
import jax
import jax.numpy as jnp
from jax import lax
from jax.experimental import pallas as pl
from jax.experimental.pallas import tpu as pltpu
from jax.sharding import PartitionSpec as P

HEADS = 8
HEAD_DIM = 64
SPARSE = 1024
SLIDES = 16
TOK = 256
FIRST = 1
ROWS = 32
MESH = pl.DeviceIdType.MESH
BF = jnp.bfloat16
F32 = jnp.float32

masked_score = -1e30


def iota(shape, dim):
    return lax.broadcasted_iota(jnp.int32, shape, dim)


def nt_dot(a, b):
    return lax.dot_general(a, b, (((1,), (1,)), ((), ())), preferred_element_type=F32)


def nn_dot(a, b):
    return lax.dot_general(a, b, (((1,), (0,)), ((), ())), preferred_element_type=F32)


def one_hot(mask):
    return jnp.where(mask, 1.0, 0.0).astype(BF)


def attend(q, parts, q_ids, k_ids):
    scores = jnp.concatenate([nt_dot(q, kv) for kv in parts], axis=1)
    scores = jnp.where(q_ids == k_ids, scores, masked_score)
    row_max = jnp.max(scores, axis=1, keepdims=True)
    expos = jnp.exp(scores - row_max)
    total = jnp.sum(expos, axis=1, keepdims=True)
    probs = expos.astype(BF)
    mixed, at = None, 0
    for kv in parts:
        term = nn_dot(probs[:, at : at + kv.shape[0]], kv)
        mixed = term if mixed is None else mixed + term
        at += kv.shape[0]
    return mixed / total, row_max + jnp.log(total)


def kernel(
    q_hbm, k_hbm, v_hbm, w_hbm, len_hbm, out_ref,
    q_ref, k_ref, v_ref, w_ref, len_ref,
    kv, qs, mkv, qmid, t_own, t_y, t_z, topkv, mid_out, top_out, mid_res, top_res,
    mixed, acc, ids_q, ids_k, k_top, v_top,
    ready, loads, s_sib, r_sib, s_yd, r_yd, s_y, r_y, s_fw, r_fw, s_mz, r_mz, s_qz, r_qz,
    s_ty, r_ty, s_tz, r_tz, s_tx, r_tx, s_mr, r_mr, s_tr, r_tr, s_mf, r_mf,
):
    outer = lax.axis_index("outer")
    inner = lax.axis_index("inner")
    x, y_lo = outer // 4, outer % 4
    z, side, core = inner // 4, (inner // 2) % 2, inner % 2
    y = side * 4 + y_lo

    def at_z(zz, c):
        return (outer, zz * 4 + side * 2 + c)

    def at_xy(xx, yy):
        return (xx * 4 + yy % 4, z * 4 + (yy // 4) * 2 + core)

    def send(src, dst, s, r, device):
        return pltpu.make_async_remote_copy(
            src_ref=src, dst_ref=dst, send_sem=s, recv_sem=r, device_id=device, device_id_type=MESH
        )

    partner = at_xy(x, (y + 4) % 8)
    sibling = at_z(z, 1 - core)
    y_to = [at_xy(x, (y + k) % 8) for k in (4, 3, 5, 2, 6, 1, 7)]
    x_to = [at_xy((x + k) % 4, y) for k in (2, 1, 3)]
    z_to = [(z + k) % 8 for k in (4, 3, 5, 2, 6, 1, 7)]

    barrier = pltpu.get_barrier_semaphore()

    def greet(devices):
        for device in devices:
            pl.semaphore_signal(barrier, inc=1, device_id=device, device_id_type=MESH)

    def on_core(device, c):
        return (device[0], device[1] - core + c)

    greet([on_core(device, 0) for device in y_to])

    @pl.when(core == 1)
    def _():
        greet([sibling])

    load = []
    for src, dst in (
        (k_hbm.at[0:16], k_top.at[0]), (k_hbm.at[TOK // 2 : TOK // 2 + 16], k_top.at[1]),
        (v_hbm.at[0:16], v_top.at[0]), (v_hbm.at[TOK // 2 : TOK // 2 + 16], v_top.at[1]),
        (k_hbm, k_ref), (v_hbm, v_ref), (q_hbm, q_ref), (len_hbm, len_ref), (w_hbm, w_ref),
    ):
        load.append(pltpu.make_async_copy(src, dst, loads.at[len(load)]))
        load[-1].start()
    zx_core1 = [at_z(zz, 1) for zz in z_to] + [on_core(device, 1) for device in x_to]
    greet(zx_core1)

    for j in range(4):
        load[j].wait()
    low = iota((32, 128), 1) < HEAD_DIM
    rows = []
    for p in range(4):
        lanes = slice(p * 128, (p + 1) * 128)
        keys = pltpu.roll(k_top[:, :, lanes].reshape(32, 128).astype(F32), 64, 1)
        vals = v_top[:, :, lanes].reshape(32, 128).astype(F32)
        rows += [jnp.where(low, vals, keys).astype(BF), jnp.where(low, keys, vals).astype(BF)]
    row, col = iota((16, TOK), 0), iota((16, TOK), 1)
    pick = one_hot(col == row // 2 * 33 + row % 2 * 16)
    tops = nn_dot(pick, jnp.concatenate(rows, axis=0)).astype(BF)
    t_own[...] = tops
    t_y[y] = tops

    @pl.when(core == 0)
    def _():
        pl.semaphore_wait(barrier, 2 * len(y_to) + 1)
        pl.semaphore_signal(ready, inc=1, device_id=sibling, device_id_type=MESH)

    @pl.when(core == 1)
    def _():
        pl.semaphore_wait(ready, 1)

    for device in y_to:
        send(t_own, t_y.at[y], s_ty, r_ty, device).start()

    row, col = iota((TOK, TOK), 0), iota((TOK, TOK), 1)
    perm = one_hot(col == 8 * (row % ROWS) + row // ROWS)
    low = iota((TOK, 128), 1) < HEAD_DIM
    load[4].wait()
    load[5].wait()
    for p in range(4):
        lanes = slice(p * 128, (p + 1) * 128)
        keys = pltpu.roll(nn_dot(perm, k_ref[:, lanes]), 64, 1)
        vals = nn_dot(perm, v_ref[:, lanes])
        kv[0, 2 * p] = jnp.where(low, vals, keys).astype(BF).reshape(8, ROWS, 128)
        kv[0, 2 * p + 1] = jnp.where(low, keys, vals).astype(BF).reshape(8, ROWS, 128)

    for h in range(HEADS):
        send(kv.at[0, h, h], kv.at[2, h, h], s_yd, r_yd, partner).start()

    def across(h):
        if h > 0:
            send(kv.at[0, h, 0:h], kv.at[2, h, 0:h], s_y.at[h], r_y.at[h], partner).start()
        if h < 7:
            send(kv.at[0, h, h + 1 : 8], kv.at[2, h, h + 1 : 8], s_y.at[h], r_y.at[h], partner).start()

    for h in range(FIRST):
        across(h)
    whole = send(kv.at[0], kv.at[1], s_sib, r_sib, sibling)
    whole.start()

    load[6].wait()
    for p in range(4):
        lanes = slice(p * 128, (p + 1) * 128)
        rows = pltpu.roll(nn_dot(perm, q_ref[:, lanes]), 64, 1) * HEAD_DIM**-0.5
        qs[2 * p] = jnp.where(low, 0.0, rows).astype(BF).reshape(8, ROWS, 128)
        qs[2 * p + 1] = jnp.where(low, rows, 0.0).astype(BF).reshape(8, ROWS, 128)

    load[7].wait()
    ends, running = [], jnp.int32(0)
    for j in range(SLIDES):
        running = running + len_ref[j]
        ends.append(running)

    def slides(positions):
        found = jnp.zeros(positions.shape, jnp.int32)
        for end in ends:
            found = found + (positions >= end).astype(jnp.int32)
        return found

    block = outer * (32 * TOK)
    first = block + inner * TOK
    r = iota((TOK, 1), 0)
    ids_q[...] = jnp.broadcast_to(slides(first + 8 * (r % ROWS) + r // ROWS), (TOK, 128))
    n = iota((1, SPARSE), 1)
    slot, n = n // TOK, n % TOK
    far, other = slot // 2, slot % 2
    device = z * 4 + (side + far - 2 * far * side) * 2 + (core + other - 2 * other * core)
    ids_k[...] = jnp.broadcast_to(
        slides(block + device * TOK + 8 * (n % ROWS) + n // ROWS), (8, SPARSE)
    )

    def own_rows():
        @pl.when(core == 1)
        def _():
            pl.semaphore_wait(barrier, 2 * len(zx_core1))
            pl.semaphore_signal(ready, inc=1, device_id=sibling, device_id_type=MESH)

        @pl.when(core == 0)
        def _():
            pl.semaphore_wait(ready, 1)

        for zz in z_to:
            send(kv.at[0, zz, zz], mkv.at[core, slot_own], s_mz, r_mz, at_z(zz, core)).start()
            send(qs.at[zz, zz], qmid.at[z], s_qz, r_qz, at_z(zz, core)).start()

    slot_own, slot_far = z * 2 + side, z * 2 + 1 - side
    pl.when(z >= 2)(own_rows)

    all_ty = send(t_y.at[0:7], t_y.at[0:7], s_ty, r_ty, sibling)
    all_ty.wait_recv()
    for h in range(FIRST, HEADS):
        across(h)

    row, col = iota((128, 128), 0), iota((128, 128), 1)
    pick = col == row // 2 % 8 * 16 + row // 16 * 2 + row % 2
    t_z[...] = nn_dot(one_hot(pick), t_y[...].reshape(128, 128)).astype(BF).reshape(8, 16, 128)

    pl.when(z < 2)(own_rows)

    slot = z * 2 + core
    for zz in z_to:
        for c in (core, 1 - core):
            send(t_z.at[zz], topkv.at[x, slot], s_tz, r_tz, at_z(zz, c)).start()
    send(t_z.at[z], topkv.at[x, slot], s_tz, r_tz, sibling).start()
    topkv[x, slot] = t_z[z]

    mkv[core, slot_own] = kv[0, z, z]
    qmid[z] = qs[z, z]
    send(kv.at[0, 0], kv.at[2, 0], s_yd, r_yd, partner).wait_recv()
    for zz in z_to:
        send(kv.at[2, zz, zz], mkv.at[core, slot_far], s_mz, r_mz, at_z(zz, core)).start()
    mkv[core, slot_far] = kv[2, z, z]

    def forward(h):
        return send(kv.at[2, h], kv.at[3, h], s_fw.at[h], r_fw.at[h], sibling)

    def arrived(h):
        send(kv.at[0, h, 0:7], kv.at[2, h, 0:7], s_y.at[h], r_y.at[h], partner).wait_recv()
        forward(h).start()

    lane_half = iota((TOK, 128), 1) // HEAD_DIM

    def local(h):
        forward(h).wait_recv()
        parts = [kv[s, h].reshape(TOK, 128) for s in range(4)]
        branch, branch_lse = attend(
            qs[h].reshape(TOK, 128), parts, ids_q[:, 0:1], ids_k[0:1, :]
        )
        mixed[h] = jnp.where(lane_half == h % 2, branch, branch_lse)

    def local_heads(start, stop):
        def body(h, _):
            arrived(h + 1)
            local(h)
            return _

        lax.fori_loop(start, stop, body, 0)

    def mix(h):
        l_at = HEAD_DIM - h % 2 * HEAD_DIM
        rows = slice(h * ROWS, (h + 1) * ROWS)
        row = iota((ROWS, 1), 0)
        own, mid, top = mixed[h, rows, :], mid_res[h], top_res[h]
        top = jnp.where(row == 0, top[0:1], top[1:2])
        lse1 = own[:, l_at : l_at + 1]
        lse2 = mid[:, l_at : l_at + 1]
        lse3 = jnp.where(row % 16 == 0, top[:, l_at : l_at + 1], masked_score)
        largest = jnp.maximum(jnp.maximum(lse1, lse2), lse3)
        f1, f2, f3 = jnp.exp(lse1 - largest), jnp.exp(lse2 - largest), jnp.exp(lse3 - largest)
        mixed[h, rows, :] = (f1 * own + f2 * mid + f3 * top) / (f1 + f2 + f3)

    row, col = iota((TOK, TOK), 0), iota((TOK, TOK), 1)
    back = one_hot(row == 8 * (col % ROWS) + col // ROWS)

    def project(p):
        rows = jnp.where(low, mixed[2 * p], mixed[2 * p + 1]).astype(BF)
        rows = nn_dot(back, rows).astype(BF)
        return nn_dot(rows, w_ref[p * 128 : (p + 1) * 128, :])

    all_tz = send(topkv.at[0, 0:15], topkv.at[0, 0:15], s_tz, r_tz, sibling)
    ahead = (7 - z) // 3
    whole.wait_recv()
    arrived(0)
    local_heads(0, ahead)
    all_tz.wait_recv()
    for device in x_to:
        send(topkv.at[x], topkv.at[x], s_tx, r_tx, device).start()

    all_mz = send(mkv.at[0, 0:14], mkv.at[0, 0:14], s_mz, r_mz, sibling)
    all_mz.wait_recv()
    share = send(mkv.at[core], mkv.at[core], s_mf, r_mf, sibling)
    share.start()
    local_heads(ahead, ahead + 1)
    share.wait_recv()
    all_qz = send(qmid.at[0:7], qmid.at[0:7], s_qz, r_qz, sibling)
    all_qz.wait_recv()
    v_low = z % 2
    mid_q = qmid[...].reshape(TOK, 128)
    r, n = iota((TOK, 1), 0), iota((1, SPARSE), 1)
    mid_ids_q = slides(block + ((r // ROWS) * 4 + side * 2 + core) * TOK + 8 * (r % ROWS) + z)
    slot = n // ROWS
    device = slot % 16 // 2 * 4 + slot % 2 * 2 + slot // 16
    mid_ids_k = slides(block + device * TOK + 8 * (n % ROWS) + z)
    branch, branch_lse = attend(mid_q, [mkv[...].reshape(SPARSE, 128)], mid_ids_q, mid_ids_k)
    holds = iota((TOK, 128), 1) // HEAD_DIM == v_low
    mid_out[...] = jnp.where(holds, branch, branch_lse).reshape(8, ROWS, 128)
    for zz in z_to:
        send(mid_out.at[zz], mid_res.at[z], s_mr, r_mr, at_z(zz, core)).start()
    mid_res[z] = mid_out[z]

    row, col = iota((64, TOK), 0), iota((64, TOK), 1)
    pick = (row % 8 < 2) & (col == row // 8 * ROWS + row % 8 * 16)
    top_q = nn_dot(one_hot(pick), mid_q).astype(BF)
    r, n = iota((64, 1), 0), iota((1, SPARSE), 1)
    top_ids_q = slides(block + ((r // 8) * 4 + side * 2 + core) * TOK + (r % 8) * 128 + z)
    far_y = n // 2 % 8
    device = (n // 256 * 4 + far_y % 4) * 32 + n // 32 % 8 * 4 + far_y // 4 * 2 + n // 16 % 2
    top_ids_k = slides(device * TOK + n % 2 * 128 + z)
    all_tx = send(topkv.at[0:3], topkv.at[0:3], s_tx, r_tx, sibling)
    all_tx.wait_recv()
    branch, branch_lse = attend(top_q, [topkv[...].reshape(SPARSE, 128)], top_ids_q, top_ids_k)
    holds = iota((64, 128), 1) // HEAD_DIM == v_low
    top_out[...] = jnp.where(holds, branch, branch_lse).reshape(8, 8, 128)
    for zz in z_to:
        send(top_out.at[zz], top_res.at[z], s_tr, r_tr, at_z(zz, core)).start()
    top_res[z] = top_out[z]

    local_heads(ahead + 1, 4)
    load[8].wait()
    all_mr = send(mid_out.at[0:7], mid_res.at[0:7], s_mr, r_mr, sibling)
    all_mr.wait_recv()
    all_tr = send(top_out.at[0:7], top_res.at[0:7], s_tr, r_tr, sibling)
    all_tr.wait_recv()
    for h in range(4):
        mix(h)
    acc[...] = project(0) + project(1)
    local_heads(4, 6)
    mix(4)
    mix(5)
    acc[...] += project(2)
    local_heads(6, 7)
    mix(6)
    local(7)
    mix(7)
    out_ref[...] = (acc[...] + project(3)).astype(BF)

    whole.wait_send()
    send(kv.at[0, 0], kv.at[2, 0], s_yd, r_yd, partner).wait_send()
    for h in range(HEADS):
        send(kv.at[0, h, 0:7], kv.at[2, h, 0:7], s_y.at[h], r_y.at[h], partner).wait_send()
        forward(h).wait_send()
    all_mz.wait_send()
    share.wait_send()
    all_qz.wait_send()
    all_ty.wait_send()
    all_tz.wait_send()
    all_tx.wait_send()
    all_mr.wait_send()
    all_tr.wait_send()


def shards(queries, keys, values, out_weight, slide_lengths):
    args = (queries, keys, values, out_weight, slide_lengths)
    dma = pltpu.SemaphoreType.DMA
    width = HEADS * HEAD_DIM
    return pl.pallas_call(
        kernel,
        out_shape=jax.ShapeDtypeStruct((TOK, out_weight.shape[1]), BF),
        in_specs=[pl.BlockSpec(memory_space=pltpu.HBM)] * 5,
        out_specs=pl.BlockSpec(memory_space=pltpu.VMEM),
        scratch_shapes=[
            pltpu.VMEM((TOK, width), BF),
            pltpu.VMEM((TOK, width), BF),
            pltpu.VMEM((TOK, width), BF),
            pltpu.VMEM(out_weight.shape, BF),
            pltpu.SMEM((SLIDES,), jnp.int32),
            pltpu.VMEM((4, HEADS, 8, ROWS, 128), BF),
            pltpu.VMEM((HEADS, 8, ROWS, 128), BF),
            pltpu.VMEM((2, 16, ROWS, 128), BF),
            pltpu.VMEM((8, ROWS, 128), BF),
            pltpu.VMEM((16, 128), BF),
            pltpu.VMEM((8, 16, 128), BF),
            pltpu.VMEM((8, 16, 128), BF),
            pltpu.VMEM((4, 16, 16, 128), BF),
            pltpu.VMEM((8, ROWS, 128), F32),
            pltpu.VMEM((8, 8, 128), F32),
            pltpu.VMEM((8, ROWS, 128), F32),
            pltpu.VMEM((8, 8, 128), F32),
            pltpu.VMEM((HEADS, TOK, 128), F32),
            pltpu.VMEM((TOK, out_weight.shape[1]), F32),
            pltpu.VMEM((TOK, 128), jnp.int32),
            pltpu.VMEM((8, SPARSE), jnp.int32),
            pltpu.VMEM((2, 16, width), BF),
            pltpu.VMEM((2, 16, width), BF),
            pltpu.SemaphoreType.REGULAR, dma((9,)), dma, dma, dma, dma, dma((8,)), dma((8,)), dma((8,)), dma((8,)),
            dma, dma, dma, dma, dma, dma, dma, dma, dma, dma, dma, dma, dma, dma, dma, dma,
        ],
        compiler_params=pltpu.CompilerParams(
            collective_id=0, has_side_effects=True, vmem_limit_bytes=48 * 1024 * 1024
        ),
        name="dilated",
    )(*[pltpu.with_memory_space_constraint(a, pltpu.HBM) for a in args])


def solution(mesh):
    rows = P(("outer", "inner"), None)
    return jax.shard_map(
        shards, mesh=mesh, in_specs=(rows, rows, rows, P(), P()), out_specs=rows, check_vma=False
    )
```

```python
import jax
import jax.numpy as jnp
from jax import lax
from jax.experimental import pallas as pl
from jax.experimental.pallas import tpu as pltpu
from jax.sharding import PartitionSpec as P

HEADS = 8
HEAD_DIM = 64
SPARSE = 1024
SLIDES = 16
TOK = 256
FIRST = 2
ROWS = 32
MESH = pl.DeviceIdType.MESH
BF = jnp.bfloat16
F32 = jnp.float32

masked_score = -1e30


def iota(shape, dim):
    return lax.broadcasted_iota(jnp.int32, shape, dim)


def nt_dot(a, b):
    return lax.dot_general(a, b, (((1,), (1,)), ((), ())), preferred_element_type=F32)


def nn_dot(a, b):
    return lax.dot_general(a, b, (((1,), (0,)), ((), ())), preferred_element_type=F32)


def one_hot(mask):
    return jnp.where(mask, 1.0, 0.0).astype(BF)


def attend_part(q, parts, q_ids, k_ids):
    scores = jnp.concatenate([nt_dot(q, kv) for kv in parts], axis=1)
    scores = jnp.where(q_ids == k_ids, scores, masked_score)
    row_max = jnp.max(scores, axis=1, keepdims=True)
    expos = jnp.exp(scores - row_max)
    total = jnp.sum(expos, axis=1, keepdims=True)
    probs = expos.astype(BF)
    mixed, at = None, 0
    for kv in parts:
        term = nn_dot(probs[:, at : at + kv.shape[0]], kv)
        mixed = term if mixed is None else mixed + term
        at += kv.shape[0]
    return mixed, row_max, total


def attend(q, parts, q_ids, k_ids):
    mixed, row_max, total = attend_part(q, parts, q_ids, k_ids)
    return mixed / total, row_max + jnp.log(total)


def kernel(
    q_hbm, k_hbm, v_hbm, len_hbm, out_ref,
    q_ref, k_ref, v_ref, len_ref,
    kv, qs, mkv, qmid, t_own, t_y, t_z, topkv, mid_out, top_out, mid_res, top_res,
    mixed, ids_q, ids_k, k_top, v_top, half_o, half_l,
    ready, loads, s_sib, r_sib, s_yd, r_yd, s_y, r_y, s_fw, r_fw, s_mz, r_mz, s_qz, r_qz,
    s_ty, r_ty, s_tz, r_tz, s_tx, r_tx, s_mr, r_mr, s_tr, r_tr, s_mf, r_mf,
):
    outer = lax.axis_index("outer")
    inner = lax.axis_index("inner")
    x, y_lo = outer // 4, outer % 4
    z, side, core = inner // 4, (inner // 2) % 2, inner % 2
    y = side * 4 + y_lo

    def at_z(zz, c):
        return (outer, zz * 4 + side * 2 + c)

    def at_xy(xx, yy):
        return (xx * 4 + yy % 4, z * 4 + (yy // 4) * 2 + core)

    def send(src, dst, s, r, device):
        return pltpu.make_async_remote_copy(
            src_ref=src, dst_ref=dst, send_sem=s, recv_sem=r, device_id=device, device_id_type=MESH
        )

    partner = at_xy(x, (y + 4) % 8)
    sibling = at_z(z, 1 - core)
    y_to = [at_xy(x, (y + k) % 8) for k in (4, 3, 5, 2, 6, 1, 7)]
    x_to = [at_xy((x + k) % 4, y) for k in (2, 1, 3)]
    z_to = [(z + k) % 8 for k in (4, 3, 5, 2, 6, 1, 7)]

    barrier = pltpu.get_barrier_semaphore()

    def greet(devices):
        for device in devices:
            pl.semaphore_signal(barrier, inc=1, device_id=device, device_id_type=MESH)

    def on_core(device, c):
        return (device[0], device[1] - core + c)

    greet([on_core(device, 0) for device in y_to])

    @pl.when(core == 1)
    def _():
        greet([sibling])

    load = []
    for src, dst in (
        (k_hbm.at[0:16], k_top.at[0]), (k_hbm.at[TOK // 2 : TOK // 2 + 16], k_top.at[1]),
        (v_hbm.at[0:16], v_top.at[0]), (v_hbm.at[TOK // 2 : TOK // 2 + 16], v_top.at[1]),
        (k_hbm, k_ref), (v_hbm, v_ref), (q_hbm, q_ref), (len_hbm, len_ref),
    ):
        load.append(pltpu.make_async_copy(src, dst, loads.at[len(load)]))
        load[-1].start()
    zx_core1 = [at_z(zz, 1) for zz in z_to] + [on_core(device, 1) for device in x_to]
    greet(zx_core1)

    for j in range(4):
        load[j].wait()
    low = iota((32, 128), 1) < HEAD_DIM
    rows = []
    for p in range(4):
        lanes = slice(p * 128, (p + 1) * 128)
        keys = pltpu.roll(k_top[:, :, lanes].reshape(32, 128).astype(F32), 64, 1)
        vals = v_top[:, :, lanes].reshape(32, 128).astype(F32)
        rows += [jnp.where(low, vals, keys).astype(BF), jnp.where(low, keys, vals).astype(BF)]
    row, col = iota((16, TOK), 0), iota((16, TOK), 1)
    pick = one_hot(col == row // 2 * 33 + row % 2 * 16)
    tops = nn_dot(pick, jnp.concatenate(rows, axis=0)).astype(BF)
    t_own[...] = tops
    t_y[y] = tops

    @pl.when(core == 0)
    def _():
        pl.semaphore_wait(barrier, 2 * len(y_to) + 1)
        pl.semaphore_signal(ready, inc=1, device_id=sibling, device_id_type=MESH)

    @pl.when(core == 1)
    def _():
        pl.semaphore_wait(ready, 1)

    for device in y_to:
        send(t_own, t_y.at[y], s_ty, r_ty, device).start()

    row, col = iota((TOK, TOK), 0), iota((TOK, TOK), 1)
    perm = one_hot(col == 8 * (row % ROWS) + row // ROWS)
    low = iota((TOK, 128), 1) < HEAD_DIM
    load[4].wait()
    load[5].wait()
    for p in range(4):
        lanes = slice(p * 128, (p + 1) * 128)
        part = perm[p * 64 : (p + 1) * 64]
        keys = pltpu.roll(nn_dot(part, k_ref[:, lanes]), 64, 1)
        vals = nn_dot(part, v_ref[:, lanes])
        kv[0, 2 * p, 2 * p] = jnp.where(low[:32], vals[:32], keys[:32]).astype(BF)
        kv[0, 2 * p + 1, 2 * p + 1] = jnp.where(low[:32], keys[32:], vals[32:]).astype(BF)
    for h in range(HEADS):
        send(kv.at[0, h, h], kv.at[2, h, h], s_yd, r_yd, partner).start()

    def keep(h, rows):
        rows = rows.astype(BF).reshape(8, ROWS, 128)
        if h > 0:
            kv[0, h, 0:h] = rows[0:h]
        if h < 7:
            kv[0, h, h + 1 : 8] = rows[h + 1 : 8]

    for p in range(4):
        lanes = slice(p * 128, (p + 1) * 128)
        keys = pltpu.roll(nn_dot(perm, k_ref[:, lanes]), 64, 1)
        vals = nn_dot(perm, v_ref[:, lanes])
        keep(2 * p, jnp.where(low, vals, keys))
        keep(2 * p + 1, jnp.where(low, keys, vals))

    def across(h):
        if h > 0:
            send(kv.at[0, h, 0:h], kv.at[2, h, 0:h], s_y.at[h], r_y.at[h], partner).start()
        if h < 7:
            send(kv.at[0, h, h + 1 : 8], kv.at[2, h, h + 1 : 8], s_y.at[h], r_y.at[h], partner).start()

    for h in range(FIRST):
        across(h)
    whole = send(kv.at[0], kv.at[1], s_sib, r_sib, sibling)
    whole.start()

    load[6].wait()
    for p in range(4):
        lanes = slice(p * 128, (p + 1) * 128)
        rows = pltpu.roll(nn_dot(perm, q_ref[:, lanes]), 64, 1) * HEAD_DIM**-0.5
        qs[2 * p] = jnp.where(low, 0.0, rows).astype(BF).reshape(8, ROWS, 128)
        qs[2 * p + 1] = jnp.where(low, rows, 0.0).astype(BF).reshape(8, ROWS, 128)

    load[7].wait()
    ends, running = [], jnp.int32(0)
    for j in range(SLIDES):
        running = running + len_ref[j]
        ends.append(running)

    def slides(positions):
        found = jnp.zeros(positions.shape, jnp.int32)
        for end in ends:
            found = found + (positions >= end).astype(jnp.int32)
        return found

    block = outer * (32 * TOK)
    first = block + inner * TOK
    r = iota((TOK, 1), 0)
    ids_q[...] = jnp.broadcast_to(slides(first + 8 * (r % ROWS) + r // ROWS), (TOK, 128))
    n = iota((1, SPARSE), 1)
    slot, n = n // TOK, n % TOK
    far, other = slot // 2, slot % 2
    device = z * 4 + (side + far - 2 * far * side) * 2 + (core + other - 2 * other * core)
    ids_k[...] = jnp.broadcast_to(
        slides(block + device * TOK + 8 * (n % ROWS) + n // ROWS), (8, SPARSE)
    )

    def own_rows():
        @pl.when(core == 1)
        def _():
            pl.semaphore_wait(barrier, 2 * len(zx_core1))
            pl.semaphore_signal(ready, inc=1, device_id=sibling, device_id_type=MESH)

        @pl.when(core == 0)
        def _():
            pl.semaphore_wait(ready, 1)

        for zz in z_to:
            send(kv.at[0, zz, zz], mkv.at[core, slot_own], s_mz, r_mz, at_z(zz, core)).start()
            send(qs.at[zz, zz], qmid.at[z], s_qz, r_qz, at_z(zz, core)).start()

    slot_own, slot_far = z * 2 + side, z * 2 + 1 - side
    pl.when(z >= 2)(own_rows)

    all_ty = send(t_y.at[0:7], t_y.at[0:7], s_ty, r_ty, sibling)
    all_ty.wait_recv()
    for h in range(FIRST, HEADS):
        across(h)

    row, col = iota((128, 128), 0), iota((128, 128), 1)
    pick = col == row // 2 % 8 * 16 + row // 16 * 2 + row % 2
    t_z[...] = nn_dot(one_hot(pick), t_y[...].reshape(128, 128)).astype(BF).reshape(8, 16, 128)

    pl.when(z < 2)(own_rows)

    slot = z * 2 + core
    for zz in z_to:
        for c in (core, 1 - core):
            send(t_z.at[zz], topkv.at[x, slot], s_tz, r_tz, at_z(zz, c)).start()
    send(t_z.at[z], topkv.at[x, slot], s_tz, r_tz, sibling).start()
    topkv[x, slot] = t_z[z]

    mkv[core, slot_own] = kv[0, z, z]
    qmid[z] = qs[z, z]
    send(kv.at[0, 0], kv.at[2, 0], s_yd, r_yd, partner).wait_recv()
    for zz in z_to:
        send(kv.at[2, zz, zz], mkv.at[core, slot_far], s_mz, r_mz, at_z(zz, core)).start()
    mkv[core, slot_far] = kv[2, z, z]

    def forward(h):
        return send(kv.at[2, h], kv.at[3, h], s_fw.at[h], r_fw.at[h], sibling)

    def arrived(h):
        send(kv.at[0, h, 0:7], kv.at[2, h, 0:7], s_y.at[h], r_y.at[h], partner).wait_recv()
        forward(h).start()

    lane_half = iota((TOK, 128), 1) // HEAD_DIM

    def local(h):
        forward(h).wait_recv()
        parts = [kv[s, h].reshape(TOK, 128) for s in range(4)]
        branch, branch_lse = attend(
            qs[h].reshape(TOK, 128), parts, ids_q[:, 0:1], ids_k[0:1, :]
        )
        mixed[h] = jnp.where(lane_half == h % 2, branch, branch_lse)

    def local_half(h, half):
        parts = [kv[2 * half + s, h].reshape(TOK, 128) for s in range(2)]
        keys = slice(half * 2 * TOK, (half + 1) * 2 * TOK)
        return attend_part(qs[h].reshape(TOK, 128), parts, ids_q[:, 0:1], ids_k[0:1, keys])

    def local_heads(start, stop):
        def body(h, _):
            arrived(h + 1)
            local(h)
            return _

        lax.fori_loop(start, stop, body, 0)

    def mix(h):
        l_at = HEAD_DIM - h % 2 * HEAD_DIM
        rows = slice(h * ROWS, (h + 1) * ROWS)
        row = iota((ROWS, 1), 0)
        own, mid, top = mixed[h, rows, :], mid_res[h].astype(F32), top_res[h]
        top = jnp.where(row == 0, top[0:1], top[1:2])
        lse1 = own[:, l_at : l_at + 1]
        lse2 = mid[:, l_at : l_at + 1] + mid[:, l_at + 1 : l_at + 2] + mid[:, l_at + 2 : l_at + 3]
        lse3 = jnp.where(row % 16 == 0, top[:, l_at : l_at + 1], masked_score)
        largest = jnp.maximum(jnp.maximum(lse1, lse2), lse3)
        f1, f2, f3 = jnp.exp(lse1 - largest), jnp.exp(lse2 - largest), jnp.exp(lse3 - largest)
        mixed[h, rows, :] = (f1 * own + f2 * mid + f3 * top) / (f1 + f2 + f3)

    row, col = iota((TOK, TOK), 0), iota((TOK, TOK), 1)
    back = one_hot(row == 8 * (col % ROWS) + col // ROWS)

    def restore(p):
        rows = jnp.where(low, mixed[2 * p], mixed[2 * p + 1]).astype(BF)
        out_ref[:, p * 128 : (p + 1) * 128] = nn_dot(back, rows).astype(BF)

    all_tz = send(topkv.at[0, 0:15], topkv.at[0, 0:15], s_tz, r_tz, sibling)
    ahead = (z <= 2).astype(jnp.int32) + (z == 0).astype(jnp.int32)
    between = jnp.where(z <= 2, ahead + 1, 0)
    before = 4 + (z <= 3).astype(jnp.int32)

    @pl.when(z <= 2)
    def _():
        whole.wait_recv()
        arrived(0)
        local_heads(0, ahead)

    all_tz.wait_recv()
    for device in x_to:
        send(topkv.at[x], topkv.at[x], s_tx, r_tx, device).start()

    all_mz = send(mkv.at[0, 0:14], mkv.at[0, 0:14], s_mz, r_mz, sibling)
    all_mz.wait_recv()
    share = send(mkv.at[core], mkv.at[core], s_mf, r_mf, sibling)
    share.start()
    local_heads(ahead, jnp.maximum(ahead, between))
    share.wait_recv()
    all_qz = send(qmid.at[0:7], qmid.at[0:7], s_qz, r_qz, sibling)
    all_qz.wait_recv()
    v_low = z % 2
    mid_q = qmid[...].reshape(TOK, 128)
    r, n = iota((TOK, 1), 0), iota((1, SPARSE), 1)
    mid_ids_q = slides(block + ((r // ROWS) * 4 + side * 2 + core) * TOK + 8 * (r % ROWS) + z)
    slot = n // ROWS
    device = slot % 16 // 2 * 4 + slot % 2 * 2 + slot // 16
    mid_ids_k = slides(block + device * TOK + 8 * (n % ROWS) + z)
    branch, branch_lse = attend(mid_q, [mkv[...].reshape(SPARSE, 128)], mid_ids_q, mid_ids_k)
    holds = iota((TOK, 128), 1) // HEAD_DIM == v_low
    third, left = [], branch_lse
    for _ in range(3):
        third.append(left.astype(BF).astype(F32))
        left = left - third[-1]
    lane = iota((TOK, 128), 1) % HEAD_DIM
    spread = jnp.where(lane == 0, third[0], jnp.where(lane == 1, third[1], third[2]))
    mid_out[...] = jnp.where(holds, branch, spread).astype(BF).reshape(8, ROWS, 128)
    for zz in z_to:
        send(mid_out.at[zz], mid_res.at[z], s_mr, r_mr, at_z(zz, core)).start()
    mid_res[z] = mid_out[z]

    @pl.when(z > 2)
    def _():
        whole.wait_recv()
        arrived(0)

    local_heads(between, between + 1)

    row, col = iota((64, TOK), 0), iota((64, TOK), 1)
    pick = (row % 8 < 2) & (col == row // 8 * ROWS + row % 8 * 16)
    top_q = nn_dot(one_hot(pick), mid_q).astype(BF)
    r, n = iota((64, 1), 0), iota((1, SPARSE), 1)
    top_ids_q = slides(block + ((r // 8) * 4 + side * 2 + core) * TOK + (r % 8) * 128 + z)
    far_y = n // 2 % 8
    device = (n // 256 * 4 + far_y % 4) * 32 + n // 32 % 8 * 4 + far_y // 4 * 2 + n // 16 % 2
    top_ids_k = slides(device * TOK + n % 2 * 128 + z)
    all_tx = send(topkv.at[0:3], topkv.at[0:3], s_tx, r_tx, sibling)
    all_tx.wait_recv()
    branch, branch_lse = attend(top_q, [topkv[...].reshape(SPARSE, 128)], top_ids_q, top_ids_k)
    holds = iota((64, 128), 1) // HEAD_DIM == v_low
    top_out[...] = jnp.where(holds, branch, branch_lse).reshape(8, 8, 128)
    for zz in z_to:
        send(top_out.at[zz], top_res.at[z], s_tr, r_tr, at_z(zz, core)).start()
    top_res[z] = top_out[z]

    local_heads(between + 1, before)
    all_mr = send(mid_out.at[0:7], mid_res.at[0:7], s_mr, r_mr, sibling)
    all_mr.wait_recv()
    all_tr = send(top_out.at[0:7], top_res.at[0:7], s_tr, r_tr, sibling)
    all_tr.wait_recv()
    for h in range(4):
        mix(h)
    restore(0)
    restore(1)
    local_heads(before, 6)
    mix(4)
    mix(5)
    restore(2)
    near, near_max, near_total = local_half(7, 0)
    half_o[...] = near
    half_l[...] = jnp.where(lane_half == 0, near_max, near_total)
    arrived(7)
    local(6)
    mix(6)
    forward(7).wait_recv()
    far, far_max, far_total = local_half(7, 1)
    near_max, near_total = half_l[:, 0:1], half_l[:, HEAD_DIM : HEAD_DIM + 1]
    row_max = jnp.maximum(near_max, far_max)
    near_part, far_part = jnp.exp(near_max - row_max), jnp.exp(far_max - row_max)
    total = near_part * near_total + far_part * far_total
    branch = (near_part * half_o[...] + far_part * far) / total
    mixed[7] = jnp.where(lane_half == 1, branch, row_max + jnp.log(total))
    mix(7)
    restore(3)

    whole.wait_send()
    send(kv.at[0, 0], kv.at[2, 0], s_yd, r_yd, partner).wait_send()
    for h in range(HEADS):
        send(kv.at[0, h, 0:7], kv.at[2, h, 0:7], s_y.at[h], r_y.at[h], partner).wait_send()
        forward(h).wait_send()
    all_mz.wait_send()
    share.wait_send()
    all_qz.wait_send()
    all_ty.wait_send()
    all_tz.wait_send()
    all_tx.wait_send()
    all_mr.wait_send()
    all_tr.wait_send()


def shards(queries, keys, values, out_weight, slide_lengths):
    args = (queries, keys, values, slide_lengths)
    dma = pltpu.SemaphoreType.DMA
    width = HEADS * HEAD_DIM
    attention = pl.pallas_call(
        kernel,
        out_shape=jax.ShapeDtypeStruct((TOK, width), BF),
        in_specs=[pl.BlockSpec(memory_space=pltpu.HBM)] * 4,
        out_specs=pl.BlockSpec(memory_space=pltpu.VMEM),
        scratch_shapes=[
            pltpu.VMEM((TOK, width), BF),
            pltpu.VMEM((TOK, width), BF),
            pltpu.VMEM((TOK, width), BF),
            pltpu.SMEM((SLIDES,), jnp.int32),
            pltpu.VMEM((4, HEADS, 8, ROWS, 128), BF),
            pltpu.VMEM((HEADS, 8, ROWS, 128), BF),
            pltpu.VMEM((2, 16, ROWS, 128), BF),
            pltpu.VMEM((8, ROWS, 128), BF),
            pltpu.VMEM((16, 128), BF),
            pltpu.VMEM((8, 16, 128), BF),
            pltpu.VMEM((8, 16, 128), BF),
            pltpu.VMEM((4, 16, 16, 128), BF),
            pltpu.VMEM((8, ROWS, 128), BF),
            pltpu.VMEM((8, 8, 128), F32),
            pltpu.VMEM((8, ROWS, 128), BF),
            pltpu.VMEM((8, 8, 128), F32),
            pltpu.VMEM((HEADS, TOK, 128), F32),
            pltpu.VMEM((TOK, 128), jnp.int32),
            pltpu.VMEM((8, SPARSE), jnp.int32),
            pltpu.VMEM((2, 16, width), BF),
            pltpu.VMEM((2, 16, width), BF),
            pltpu.VMEM((TOK, 128), F32),
            pltpu.VMEM((TOK, 128), F32),
            pltpu.SemaphoreType.REGULAR, dma((8,)), dma, dma, dma, dma, dma((8,)), dma((8,)), dma((8,)), dma((8,)),
            dma, dma, dma, dma, dma, dma, dma, dma, dma, dma, dma, dma, dma, dma, dma, dma,
        ],
        compiler_params=pltpu.CompilerParams(
            collective_id=0, has_side_effects=True, vmem_limit_bytes=48 * 1024 * 1024
        ),
        name="dilated",
    )(*[pltpu.with_memory_space_constraint(a, pltpu.HBM) for a in args])
    return jnp.dot(attention, out_weight, preferred_element_type=F32).astype(BF)


def solution(mesh):
    rows = P(("outer", "inner"), None)
    return jax.shard_map(
        shards, mesh=mesh, in_specs=(rows, rows, rows, P(), P()), out_specs=rows, check_vma=False
    )
```

```python
import jax
import jax.numpy as jnp
from jax import lax
from jax.experimental import pallas as pl
from jax.experimental.pallas import tpu as pltpu
from jax.sharding import PartitionSpec as P

HEADS = 8
HEAD_DIM = 64
SPARSE = 1024
SLIDES = 16
TOK = 256
FIRST = 2
ROWS = 32
MESH = pl.DeviceIdType.MESH
BF = jnp.bfloat16
F32 = jnp.float32

masked_score = -1e30


def iota(shape, dim):
    return lax.broadcasted_iota(jnp.int32, shape, dim)


def nt_dot(a, b):
    return lax.dot_general(a, b, (((1,), (1,)), ((), ())), preferred_element_type=F32)


def nn_dot(a, b):
    return lax.dot_general(a, b, (((1,), (0,)), ((), ())), preferred_element_type=F32)


def one_hot(mask):
    return jnp.where(mask, 1.0, 0.0).astype(BF)


def attend_part(q, parts, q_ids, k_ids):
    scores = jnp.concatenate([nt_dot(q, kv) for kv in parts], axis=1)
    scores = jnp.where(q_ids == k_ids, scores, masked_score)
    row_max = jnp.max(scores, axis=1, keepdims=True)
    expos = jnp.exp(scores - row_max)
    total = jnp.sum(expos, axis=1, keepdims=True)
    probs = expos.astype(BF)
    mixed, at = None, 0
    for kv in parts:
        term = nn_dot(probs[:, at : at + kv.shape[0]], kv)
        mixed = term if mixed is None else mixed + term
        at += kv.shape[0]
    return mixed, row_max, total


def attend(q, parts, q_ids, k_ids):
    mixed, row_max, total = attend_part(q, parts, q_ids, k_ids)
    return mixed / total, row_max + jnp.log(total)


def kernel(
    q_hbm, k_hbm, v_hbm, len_hbm, out_ref,
    q_ref, k_ref, v_ref, len_ref,
    kv, qs, mkv, qmid, t_own, t_y, t_z, topkv, mid_out, top_out, mid_res, top_res,
    mixed, ids_q, ids_k, k_top, v_top, half_o, half_l,
    ready, loads, s_sib, r_sib, s_yd, r_yd, s_y, r_y, s_fw, r_fw, s_mz, r_mz, s_qz, r_qz,
    s_ty, r_ty, s_tz, r_tz, s_tx, r_tx, s_mr, r_mr, s_tr, r_tr, s_mf, r_mf,
):
    outer = lax.axis_index("outer")
    inner = lax.axis_index("inner")
    x, y_lo = outer // 4, outer % 4
    z, side, core = inner // 4, (inner // 2) % 2, inner % 2
    y = side * 4 + y_lo

    def at_z(zz, c):
        return (outer, zz * 4 + side * 2 + c)

    def at_xy(xx, yy):
        return (xx * 4 + yy % 4, z * 4 + (yy // 4) * 2 + core)

    def send(src, dst, s, r, device):
        return pltpu.make_async_remote_copy(
            src_ref=src, dst_ref=dst, send_sem=s, recv_sem=r, device_id=device, device_id_type=MESH
        )

    partner = at_xy(x, (y + 4) % 8)
    sibling = at_z(z, 1 - core)
    y_to = [at_xy(x, (y + k) % 8) for k in (4, 3, 5, 2, 6, 1, 7)]
    x_to = [at_xy((x + k) % 4, y) for k in (2, 1, 3)]
    z_to = [(z + k) % 8 for k in (4, 3, 5, 2, 6, 1, 7)]

    barrier = pltpu.get_barrier_semaphore()

    def greet(devices):
        for device in devices:
            pl.semaphore_signal(barrier, inc=1, device_id=device, device_id_type=MESH)

    def on_core(device, c):
        return (device[0], device[1] - core + c)

    greet([on_core(device, 0) for device in y_to])

    @pl.when(core == 1)
    def _():
        greet([sibling])

    load = []
    for src, dst in (
        (k_hbm.at[0:16], k_top.at[0]), (k_hbm.at[TOK // 2 : TOK // 2 + 16], k_top.at[1]),
        (v_hbm.at[0:16], v_top.at[0]), (v_hbm.at[TOK // 2 : TOK // 2 + 16], v_top.at[1]),
        (k_hbm, k_ref), (v_hbm, v_ref), (q_hbm, q_ref), (len_hbm, len_ref),
    ):
        load.append(pltpu.make_async_copy(src, dst, loads.at[len(load)]))
        load[-1].start()
    zx_core1 = [at_z(zz, 1) for zz in z_to] + [on_core(device, 1) for device in x_to]
    greet(zx_core1)

    for j in range(4):
        load[j].wait()
    low = iota((32, 128), 1) < HEAD_DIM
    rows = []
    for p in range(4):
        lanes = slice(p * 128, (p + 1) * 128)
        keys = pltpu.roll(k_top[:, :, lanes].reshape(32, 128).astype(F32), 64, 1)
        vals = v_top[:, :, lanes].reshape(32, 128).astype(F32)
        rows += [jnp.where(low, vals, keys).astype(BF), jnp.where(low, keys, vals).astype(BF)]
    row, col = iota((16, TOK), 0), iota((16, TOK), 1)
    pick = one_hot(col == row // 2 * 33 + row % 2 * 16)
    tops = nn_dot(pick, jnp.concatenate(rows, axis=0)).astype(BF)
    t_own[...] = tops
    t_y[y] = tops

    @pl.when(core == 0)
    def _():
        pl.semaphore_wait(barrier, 2 * len(y_to) + 1)
        pl.semaphore_signal(ready, inc=1, device_id=sibling, device_id_type=MESH)

    @pl.when(core == 1)
    def _():
        pl.semaphore_wait(ready, 1)

    for device in y_to:
        send(t_own, t_y.at[y], s_ty, r_ty, device).start()

    row, col = iota((TOK, TOK), 0), iota((TOK, TOK), 1)
    perm = one_hot(col == 8 * (row % ROWS) + row // ROWS)
    low = iota((TOK, 128), 1) < HEAD_DIM
    load[4].wait()
    load[5].wait()
    for p in range(4):
        lanes = slice(p * 128, (p + 1) * 128)
        part = perm[p * 64 : (p + 1) * 64]
        keys = pltpu.roll(nn_dot(part, k_ref[:, lanes]), 64, 1)
        vals = nn_dot(part, v_ref[:, lanes])
        kv[0, 2 * p, 2 * p] = jnp.where(low[:32], vals[:32], keys[:32]).astype(BF)
        kv[0, 2 * p + 1, 2 * p + 1] = jnp.where(low[:32], keys[32:], vals[32:]).astype(BF)
    for h in range(HEADS):
        send(kv.at[0, h, h], kv.at[2, h, h], s_yd, r_yd, partner).start()

    def keep(h, rows):
        rows = rows.astype(BF).reshape(8, ROWS, 128)
        if h > 0:
            kv[0, h, 0:h] = rows[0:h]
        if h < 7:
            kv[0, h, h + 1 : 8] = rows[h + 1 : 8]

    for p in range(4):
        lanes = slice(p * 128, (p + 1) * 128)
        keys = pltpu.roll(nn_dot(perm, k_ref[:, lanes]), 64, 1)
        vals = nn_dot(perm, v_ref[:, lanes])
        keep(2 * p, jnp.where(low, vals, keys))
        keep(2 * p + 1, jnp.where(low, keys, vals))

    def across(h):
        if h > 0:
            send(kv.at[0, h, 0:h], kv.at[2, h, 0:h], s_y.at[h], r_y.at[h], partner).start()
        if h < 7:
            send(kv.at[0, h, h + 1 : 8], kv.at[2, h, h + 1 : 8], s_y.at[h], r_y.at[h], partner).start()

    for h in range(FIRST):
        across(h)
    whole = send(kv.at[0], kv.at[1], s_sib, r_sib, sibling)
    whole.start()

    load[6].wait()
    for p in range(4):
        lanes = slice(p * 128, (p + 1) * 128)
        rows = pltpu.roll(nn_dot(perm, q_ref[:, lanes]), 64, 1) * HEAD_DIM**-0.5
        qs[2 * p] = jnp.where(low, 0.0, rows).astype(BF).reshape(8, ROWS, 128)
        qs[2 * p + 1] = jnp.where(low, rows, 0.0).astype(BF).reshape(8, ROWS, 128)

    load[7].wait()
    ends, running = [], jnp.int32(0)
    for j in range(SLIDES):
        running = running + len_ref[j]
        ends.append(running)

    def slides(positions):
        found = jnp.zeros(positions.shape, jnp.int32)
        for end in ends:
            found = found + (positions >= end).astype(jnp.int32)
        return found

    block = outer * (32 * TOK)
    first = block + inner * TOK
    r = iota((TOK, 1), 0)
    ids_q[...] = jnp.broadcast_to(slides(first + 8 * (r % ROWS) + r // ROWS), (TOK, 128))
    n = iota((1, SPARSE), 1)
    slot, n = n // TOK, n % TOK
    far, other = slot // 2, slot % 2
    device = z * 4 + (side + far - 2 * far * side) * 2 + (core + other - 2 * other * core)
    ids_k[...] = jnp.broadcast_to(
        slides(block + device * TOK + 8 * (n % ROWS) + n // ROWS), (8, SPARSE)
    )

    def own_rows():
        @pl.when(core == 1)
        def _():
            pl.semaphore_wait(barrier, 2 * len(zx_core1))
            pl.semaphore_signal(ready, inc=1, device_id=sibling, device_id_type=MESH)

        @pl.when(core == 0)
        def _():
            pl.semaphore_wait(ready, 1)

        for zz in z_to:
            send(kv.at[0, zz, zz], mkv.at[core, slot_own], s_mz, r_mz, at_z(zz, core)).start()
            send(qs.at[zz, zz], qmid.at[z], s_qz, r_qz, at_z(zz, core)).start()

    slot_own, slot_far = z * 2 + side, z * 2 + 1 - side
    pl.when(z >= 2)(own_rows)

    all_ty = send(t_y.at[0:7], t_y.at[0:7], s_ty, r_ty, sibling)
    all_ty.wait_recv()
    for h in range(FIRST, HEADS):
        across(h)

    row, col = iota((128, 128), 0), iota((128, 128), 1)
    pick = col == row // 2 % 8 * 16 + row // 16 * 2 + row % 2
    t_z[...] = nn_dot(one_hot(pick), t_y[...].reshape(128, 128)).astype(BF).reshape(8, 16, 128)

    pl.when(z < 2)(own_rows)

    slot = z * 2 + core
    for zz in z_to:
        for c in (core, 1 - core):
            send(t_z.at[zz], topkv.at[x, slot], s_tz, r_tz, at_z(zz, c)).start()
    send(t_z.at[z], topkv.at[x, slot], s_tz, r_tz, sibling).start()
    topkv[x, slot] = t_z[z]

    mkv[core, slot_own] = kv[0, z, z]
    qmid[z] = qs[z, z]
    send(kv.at[0, 0], kv.at[2, 0], s_yd, r_yd, partner).wait_recv()
    for zz in z_to:
        send(kv.at[2, zz, zz], mkv.at[core, slot_far], s_mz, r_mz, at_z(zz, core)).start()
    mkv[core, slot_far] = kv[2, z, z]

    def forward(h):
        return send(kv.at[2, h], kv.at[3, h], s_fw.at[h], r_fw.at[h], sibling)

    def arrived(h):
        send(kv.at[0, h, 0:7], kv.at[2, h, 0:7], s_y.at[h], r_y.at[h], partner).wait_recv()
        forward(h).start()

    lane_half = iota((TOK, 128), 1) // HEAD_DIM

    def local(h):
        forward(h).wait_recv()
        parts = [kv[s, h].reshape(TOK, 128) for s in range(4)]
        branch, branch_lse = attend(
            qs[h].reshape(TOK, 128), parts, ids_q[:, 0:1], ids_k[0:1, :]
        )
        mixed[h] = jnp.where(lane_half == h % 2, branch, branch_lse)

    def local_half(h, half):
        parts = [kv[2 * half + s, h].reshape(TOK, 128) for s in range(2)]
        keys = slice(half * 2 * TOK, (half + 1) * 2 * TOK)
        return attend_part(qs[h].reshape(TOK, 128), parts, ids_q[:, 0:1], ids_k[0:1, keys])

    def local_heads(start, stop):
        def body(h, _):
            arrived(h + 1)
            local(h)
            return _

        lax.fori_loop(start, stop, body, 0)

    def mix(h):
        l_at = HEAD_DIM - h % 2 * HEAD_DIM
        rows = slice(h * ROWS, (h + 1) * ROWS)
        row = iota((ROWS, 1), 0)
        own, mid, top = mixed[h, rows, :], mid_res[h].astype(F32), top_res[h]
        top = jnp.where(row == 0, top[0:1], top[1:2])
        lse1 = own[:, l_at : l_at + 1]
        lse2 = mid[:, l_at : l_at + 1] + mid[:, l_at + 1 : l_at + 2] + mid[:, l_at + 2 : l_at + 3]
        lse3 = jnp.where(row % 16 == 0, top[:, l_at : l_at + 1], masked_score)
        largest = jnp.maximum(jnp.maximum(lse1, lse2), lse3)
        f1, f2, f3 = jnp.exp(lse1 - largest), jnp.exp(lse2 - largest), jnp.exp(lse3 - largest)
        mixed[h, rows, :] = (f1 * own + f2 * mid + f3 * top) / (f1 + f2 + f3)

    row, col = iota((TOK, TOK), 0), iota((TOK, TOK), 1)
    back = one_hot(row == 8 * (col % ROWS) + col // ROWS)

    def restore(p):
        rows = jnp.where(low, mixed[2 * p], mixed[2 * p + 1]).astype(BF)
        out_ref[:, p * 128 : (p + 1) * 128] = nn_dot(back, rows).astype(BF)

    all_tz = send(topkv.at[0, 0:15], topkv.at[0, 0:15], s_tz, r_tz, sibling)
    two = (z == 0) & (x > 0)
    start = (z <= 2).astype(jnp.int32) + two.astype(jnp.int32)
    late = z > 3
    before = 5 - late.astype(jnp.int32)

    @pl.when(z <= 2)
    def _():
        whole.wait_recv()
        arrived(0)
        local(0)

    @pl.when(two)
    def _():
        arrived(1)
        local(1)

    all_tz.wait_recv()
    for device in x_to:
        send(topkv.at[x], topkv.at[x], s_tx, r_tx, device).start()

    all_mz = send(mkv.at[0, 0:14], mkv.at[0, 0:14], s_mz, r_mz, sibling)
    all_mz.wait_recv()
    share = send(mkv.at[core], mkv.at[core], s_mf, r_mf, sibling)
    share.start()
    share.wait_recv()
    all_qz = send(qmid.at[0:7], qmid.at[0:7], s_qz, r_qz, sibling)
    all_qz.wait_recv()
    v_low = z % 2
    mid_q = qmid[...].reshape(TOK, 128)
    r, n = iota((TOK, 1), 0), iota((1, SPARSE), 1)
    mid_ids_q = slides(block + ((r // ROWS) * 4 + side * 2 + core) * TOK + 8 * (r % ROWS) + z)
    slot = n // ROWS
    device = slot % 16 // 2 * 4 + slot % 2 * 2 + slot // 16
    mid_ids_k = slides(block + device * TOK + 8 * (n % ROWS) + z)
    branch, branch_lse = attend(mid_q, [mkv[...].reshape(SPARSE, 128)], mid_ids_q, mid_ids_k)
    holds = iota((TOK, 128), 1) // HEAD_DIM == v_low
    third, left = [], branch_lse
    for _ in range(3):
        third.append(left.astype(BF).astype(F32))
        left = left - third[-1]
    lane = iota((TOK, 128), 1) % HEAD_DIM
    spread = jnp.where(lane == 0, third[0], jnp.where(lane == 1, third[1], third[2]))
    mid_out[...] = jnp.where(holds, branch, spread).astype(BF).reshape(8, ROWS, 128)
    for zz in z_to:
        send(mid_out.at[zz], mid_res.at[z], s_mr, r_mr, at_z(zz, core)).start()
    mid_res[z] = mid_out[z]

    @pl.when(z > 2)
    def _():
        whole.wait_recv()

    arrived(start)
    local_heads(start, start + 1)

    row, col = iota((64, TOK), 0), iota((64, TOK), 1)
    pick = (row % 8 < 2) & (col == row // 8 * ROWS + row % 8 * 16)
    top_q = nn_dot(one_hot(pick), mid_q).astype(BF)
    r, n = iota((64, 1), 0), iota((1, SPARSE), 1)
    top_ids_q = slides(block + ((r // 8) * 4 + side * 2 + core) * TOK + (r % 8) * 128 + z)
    far_y = n // 2 % 8
    device = (n // 256 * 4 + far_y % 4) * 32 + n // 32 % 8 * 4 + far_y // 4 * 2 + n // 16 % 2
    top_ids_k = slides(device * TOK + n % 2 * 128 + z)
    all_tx = send(topkv.at[0:3], topkv.at[0:3], s_tx, r_tx, sibling)
    all_tx.wait_recv()
    branch, branch_lse = attend(top_q, [topkv[...].reshape(SPARSE, 128)], top_ids_q, top_ids_k)
    holds = iota((64, 128), 1) // HEAD_DIM == v_low
    top_out[...] = jnp.where(holds, branch, branch_lse).reshape(8, 8, 128)
    for zz in z_to:
        send(top_out.at[zz], top_res.at[z], s_tr, r_tr, at_z(zz, core)).start()
    top_res[z] = top_out[z]

    local_heads(start + 1, before)
    local(before)
    all_mr = send(mid_out.at[0:7], mid_res.at[0:7], s_mr, r_mr, sibling)
    all_mr.wait_recv()
    all_tr = send(top_out.at[0:7], top_res.at[0:7], s_tr, r_tr, sibling)
    all_tr.wait_recv()
    for h in range(4):
        mix(h)
    restore(0)
    restore(1)

    @pl.when(late)
    def _():
        arrived(5)
        local(5)

    arrived(6)
    mix(4)
    mix(5)
    restore(2)
    near, near_max, near_total = local_half(7, 0)
    half_o[...] = near
    half_l[...] = jnp.where(lane_half == 0, near_max, near_total)
    arrived(7)
    local(6)
    mix(6)
    forward(7).wait_recv()
    far, far_max, far_total = local_half(7, 1)
    near_max, near_total = half_l[:, 0:1], half_l[:, HEAD_DIM : HEAD_DIM + 1]
    row_max = jnp.maximum(near_max, far_max)
    near_part, far_part = jnp.exp(near_max - row_max), jnp.exp(far_max - row_max)
    total = near_part * near_total + far_part * far_total
    branch = (near_part * half_o[...] + far_part * far) / total
    mixed[7] = jnp.where(lane_half == 1, branch, row_max + jnp.log(total))
    mix(7)
    restore(3)

    whole.wait_send()
    send(kv.at[0, 0], kv.at[2, 0], s_yd, r_yd, partner).wait_send()
    for h in range(HEADS):
        send(kv.at[0, h, 0:7], kv.at[2, h, 0:7], s_y.at[h], r_y.at[h], partner).wait_send()
        forward(h).wait_send()
    all_mz.wait_send()
    share.wait_send()
    all_qz.wait_send()
    all_ty.wait_send()
    all_tz.wait_send()
    all_tx.wait_send()
    all_mr.wait_send()
    all_tr.wait_send()


def shards(queries, keys, values, out_weight, slide_lengths):
    args = (queries, keys, values, slide_lengths)
    dma = pltpu.SemaphoreType.DMA
    width = HEADS * HEAD_DIM
    attention = pl.pallas_call(
        kernel,
        out_shape=jax.ShapeDtypeStruct((TOK, width), BF),
        in_specs=[pl.BlockSpec(memory_space=pltpu.HBM)] * 4,
        out_specs=pl.BlockSpec(memory_space=pltpu.VMEM),
        scratch_shapes=[
            pltpu.VMEM((TOK, width), BF),
            pltpu.VMEM((TOK, width), BF),
            pltpu.VMEM((TOK, width), BF),
            pltpu.SMEM((SLIDES,), jnp.int32),
            pltpu.VMEM((4, HEADS, 8, ROWS, 128), BF),
            pltpu.VMEM((HEADS, 8, ROWS, 128), BF),
            pltpu.VMEM((2, 16, ROWS, 128), BF),
            pltpu.VMEM((8, ROWS, 128), BF),
            pltpu.VMEM((16, 128), BF),
            pltpu.VMEM((8, 16, 128), BF),
            pltpu.VMEM((8, 16, 128), BF),
            pltpu.VMEM((4, 16, 16, 128), BF),
            pltpu.VMEM((8, ROWS, 128), BF),
            pltpu.VMEM((8, 8, 128), F32),
            pltpu.VMEM((8, ROWS, 128), BF),
            pltpu.VMEM((8, 8, 128), F32),
            pltpu.VMEM((HEADS, TOK, 128), F32),
            pltpu.VMEM((TOK, 128), jnp.int32),
            pltpu.VMEM((8, SPARSE), jnp.int32),
            pltpu.VMEM((2, 16, width), BF),
            pltpu.VMEM((2, 16, width), BF),
            pltpu.VMEM((TOK, 128), F32),
            pltpu.VMEM((TOK, 128), F32),
            pltpu.SemaphoreType.REGULAR, dma((8,)), dma, dma, dma, dma, dma((8,)), dma((8,)), dma((8,)), dma((8,)),
            dma, dma, dma, dma, dma, dma, dma, dma, dma, dma, dma, dma, dma, dma, dma, dma,
        ],
        compiler_params=pltpu.CompilerParams(
            collective_id=0, has_side_effects=True, vmem_limit_bytes=48 * 1024 * 1024
        ),
        name="dilated",
    )(*[pltpu.with_memory_space_constraint(a, pltpu.HBM) for a in args])
    return jnp.dot(attention, out_weight, preferred_element_type=F32).astype(BF)


def solution(mesh):
    rows = P(("outer", "inner"), None)
    return jax.shard_map(
        shards, mesh=mesh, in_specs=(rows, rows, rows, P(), P()), out_specs=rows, check_vma=False
    )
```

```python
import jax
import jax.numpy as jnp
from jax import lax
from jax.experimental import pallas as pl
from jax.experimental.pallas import tpu as pltpu
from jax.sharding import PartitionSpec as P

HEADS = 8
HEAD_DIM = 64
SPARSE = 1024
SLIDES = 16
TOK = 256
FIRST = 2
ROWS = 32
MESH = pl.DeviceIdType.MESH
BF = jnp.bfloat16
F32 = jnp.float32

masked_score = -1e30


def iota(shape, dim):
    return lax.broadcasted_iota(jnp.int32, shape, dim)


def nt_dot(a, b):
    return lax.dot_general(a, b, (((1,), (1,)), ((), ())), preferred_element_type=F32)


def nn_dot(a, b):
    return lax.dot_general(a, b, (((1,), (0,)), ((), ())), preferred_element_type=F32)


def one_hot(mask):
    return jnp.where(mask, 1.0, 0.0).astype(BF)


def attend(q, parts, q_ids, k_ids):
    scores = jnp.concatenate([nt_dot(q, kv) for kv in parts], axis=1)
    scores = jnp.where(q_ids == k_ids, scores, masked_score)
    row_max = jnp.max(scores, axis=1, keepdims=True)
    expos = jnp.exp(scores - row_max)
    total = jnp.sum(expos, axis=1, keepdims=True)
    probs = expos.astype(BF)
    mixed, at = None, 0
    for kv in parts:
        term = nn_dot(probs[:, at : at + kv.shape[0]], kv)
        mixed = term if mixed is None else mixed + term
        at += kv.shape[0]
    return mixed / total, row_max + jnp.log(total)


def kernel(
    q_hbm, k_hbm, v_hbm, len_hbm, out_ref,
    q_ref, k_ref, v_ref, len_ref,
    kv, qs, mkv, qmid, t_own, t_y, t_z, topkv, mid_out, top_out, mid_res, top_res,
    mixed, ids_q, ids_k, k_top, v_top,
    ready, loads, s_sib, r_sib, s_yd, r_yd, s_y, r_y, s_fw, r_fw, s_mz, r_mz, s_qz, r_qz,
    s_ty, r_ty, s_tz, r_tz, s_tx, r_tx, s_mr, r_mr, s_tr, r_tr, s_mf, r_mf,
):
    outer = lax.axis_index("outer")
    inner = lax.axis_index("inner")
    x, y_lo = outer // 4, outer % 4
    z, side, core = inner // 4, (inner // 2) % 2, inner % 2
    y = side * 4 + y_lo

    def at_z(zz, c):
        return (outer, zz * 4 + side * 2 + c)

    def at_xy(xx, yy):
        return (xx * 4 + yy % 4, z * 4 + (yy // 4) * 2 + core)

    def send(src, dst, s, r, device):
        return pltpu.make_async_remote_copy(
            src_ref=src, dst_ref=dst, send_sem=s, recv_sem=r, device_id=device, device_id_type=MESH
        )

    partner = at_xy(x, (y + 4) % 8)
    sibling = at_z(z, 1 - core)
    y_to = [at_xy(x, (y + k) % 8) for k in (4, 3, 5, 2, 6, 1, 7)]
    x_to = [at_xy((x + k) % 4, y) for k in (2, 1, 3)]
    z_to = [(z + k) % 8 for k in (4, 3, 5, 2, 6, 1, 7)]

    barrier = pltpu.get_barrier_semaphore()

    def greet(devices):
        for device in devices:
            pl.semaphore_signal(barrier, inc=1, device_id=device, device_id_type=MESH)

    def on_core(device, c):
        return (device[0], device[1] - core + c)

    greet([on_core(device, 0) for device in y_to])

    @pl.when(core == 1)
    def _():
        greet([sibling])

    load = []
    for src, dst in (
        (k_hbm.at[0:16], k_top.at[0]), (k_hbm.at[TOK // 2 : TOK // 2 + 16], k_top.at[1]),
        (v_hbm.at[0:16], v_top.at[0]), (v_hbm.at[TOK // 2 : TOK // 2 + 16], v_top.at[1]),
        (k_hbm, k_ref), (v_hbm, v_ref), (q_hbm, q_ref), (len_hbm, len_ref),
    ):
        load.append(pltpu.make_async_copy(src, dst, loads.at[len(load)]))
        load[-1].start()
    zx_core1 = [at_z(zz, 1) for zz in z_to] + [on_core(device, 1) for device in x_to]
    greet(zx_core1)

    for j in range(4):
        load[j].wait()
    low = iota((32, 128), 1) < HEAD_DIM
    rows = []
    for p in range(4):
        lanes = slice(p * 128, (p + 1) * 128)
        keys = pltpu.roll(k_top[:, :, lanes].reshape(32, 128).astype(F32), 64, 1)
        vals = v_top[:, :, lanes].reshape(32, 128).astype(F32)
        rows += [jnp.where(low, vals, keys).astype(BF), jnp.where(low, keys, vals).astype(BF)]
    row, col = iota((16, TOK), 0), iota((16, TOK), 1)
    pick = one_hot(col == row // 2 * 33 + row % 2 * 16)
    tops = nn_dot(pick, jnp.concatenate(rows, axis=0)).astype(BF)
    t_own[...] = tops
    t_y[y] = tops

    @pl.when(core == 0)
    def _():
        pl.semaphore_wait(barrier, 2 * len(y_to) + 1)
        pl.semaphore_signal(ready, inc=1, device_id=sibling, device_id_type=MESH)

    @pl.when(core == 1)
    def _():
        pl.semaphore_wait(ready, 1)

    for device in y_to:
        send(t_own, t_y.at[y], s_ty, r_ty, device).start()

    row, col = iota((TOK, TOK), 0), iota((TOK, TOK), 1)
    perm = one_hot(col == 8 * (row % ROWS) + row // ROWS)
    low = iota((TOK, 128), 1) < HEAD_DIM
    load[4].wait()
    load[5].wait()
    for p in range(4):
        lanes = slice(p * 128, (p + 1) * 128)
        part = perm[p * 64 : (p + 1) * 64]
        keys = pltpu.roll(nn_dot(part, k_ref[:, lanes]), 64, 1)
        vals = nn_dot(part, v_ref[:, lanes])
        kv[0, 2 * p, 2 * p] = jnp.where(low[:32], vals[:32], keys[:32]).astype(BF)
        kv[0, 2 * p + 1, 2 * p + 1] = jnp.where(low[:32], keys[32:], vals[32:]).astype(BF)
    for h in range(HEADS):
        send(kv.at[0, h, h], kv.at[2, h, h], s_yd, r_yd, partner).start()

    def keep(h, rows):
        rows = rows.astype(BF).reshape(8, ROWS, 128)
        if h > 0:
            kv[0, h, 0:h] = rows[0:h]
        if h < 7:
            kv[0, h, h + 1 : 8] = rows[h + 1 : 8]

    for p in range(4):
        lanes = slice(p * 128, (p + 1) * 128)
        keys = pltpu.roll(nn_dot(perm, k_ref[:, lanes]), 64, 1)
        vals = nn_dot(perm, v_ref[:, lanes])
        keep(2 * p, jnp.where(low, vals, keys))
        keep(2 * p + 1, jnp.where(low, keys, vals))

    def across(h):
        if h > 0:
            send(kv.at[0, h, 0:h], kv.at[2, h, 0:h], s_y.at[h], r_y.at[h], partner).start()
        if h < 7:
            send(kv.at[0, h, h + 1 : 8], kv.at[2, h, h + 1 : 8], s_y.at[h], r_y.at[h], partner).start()

    for h in range(FIRST):
        across(h)
    whole = send(kv.at[0], kv.at[1], s_sib, r_sib, sibling)
    whole.start()

    load[6].wait()
    for p in range(4):
        lanes = slice(p * 128, (p + 1) * 128)
        rows = pltpu.roll(nn_dot(perm, q_ref[:, lanes]), 64, 1) * HEAD_DIM**-0.5
        qs[2 * p] = jnp.where(low, 0.0, rows).astype(BF).reshape(8, ROWS, 128)
        qs[2 * p + 1] = jnp.where(low, rows, 0.0).astype(BF).reshape(8, ROWS, 128)

    load[7].wait()
    ends, running = [], jnp.int32(0)
    for j in range(SLIDES):
        running = running + len_ref[j]
        ends.append(running)

    def slides(positions):
        found = jnp.zeros(positions.shape, jnp.int32)
        for end in ends:
            found = found + (positions >= end).astype(jnp.int32)
        return found

    block = outer * (32 * TOK)
    first = block + inner * TOK
    r = iota((TOK, 1), 0)
    ids_q[...] = jnp.broadcast_to(slides(first + 8 * (r % ROWS) + r // ROWS), (TOK, 128))
    n = iota((1, SPARSE), 1)
    slot, n = n // TOK, n % TOK
    far, other = slot // 2, slot % 2
    device = z * 4 + (side + far - 2 * far * side) * 2 + (core + other - 2 * other * core)
    ids_k[...] = jnp.broadcast_to(
        slides(block + device * TOK + 8 * (n % ROWS) + n // ROWS), (8, SPARSE)
    )

    def own_rows():
        @pl.when(core == 1)
        def _():
            pl.semaphore_wait(barrier, 2 * len(zx_core1))
            pl.semaphore_signal(ready, inc=1, device_id=sibling, device_id_type=MESH)

        @pl.when(core == 0)
        def _():
            pl.semaphore_wait(ready, 1)

        for zz in z_to:
            send(kv.at[0, zz, zz], mkv.at[core, slot_own], s_mz, r_mz, at_z(zz, core)).start()
            send(qs.at[zz, zz], qmid.at[z], s_qz, r_qz, at_z(zz, core)).start()

    slot_own, slot_far = z * 2 + side, z * 2 + 1 - side
    pl.when(z >= 2)(own_rows)

    all_ty = send(t_y.at[0:7], t_y.at[0:7], s_ty, r_ty, sibling)
    all_ty.wait_recv()
    for h in range(FIRST, HEADS):
        across(h)

    row, col = iota((128, 128), 0), iota((128, 128), 1)
    pick = col == row // 2 % 8 * 16 + row // 16 * 2 + row % 2
    t_z[...] = nn_dot(one_hot(pick), t_y[...].reshape(128, 128)).astype(BF).reshape(8, 16, 128)

    pl.when(z < 2)(own_rows)

    slot = z * 2 + core
    for zz in z_to:
        for c in (core, 1 - core):
            send(t_z.at[zz], topkv.at[x, slot], s_tz, r_tz, at_z(zz, c)).start()
    send(t_z.at[z], topkv.at[x, slot], s_tz, r_tz, sibling).start()
    topkv[x, slot] = t_z[z]

    mkv[core, slot_own] = kv[0, z, z]
    qmid[z] = qs[z, z]
    send(kv.at[0, 0], kv.at[2, 0], s_yd, r_yd, partner).wait_recv()
    for zz in z_to:
        send(kv.at[2, zz, zz], mkv.at[core, slot_far], s_mz, r_mz, at_z(zz, core)).start()
    mkv[core, slot_far] = kv[2, z, z]

    def forward(h):
        return send(kv.at[2, h], kv.at[3, h], s_fw.at[h], r_fw.at[h], sibling)

    def arrived(h):
        send(kv.at[0, h, 0:7], kv.at[2, h, 0:7], s_y.at[h], r_y.at[h], partner).wait_recv()
        forward(h).start()

    lane_half = iota((TOK, 128), 1) // HEAD_DIM

    def local(h):
        forward(h).wait_recv()
        parts = [kv[s, h].reshape(TOK, 128) for s in range(4)]
        branch, branch_lse = attend(
            qs[h].reshape(TOK, 128), parts, ids_q[:, 0:1], ids_k[0:1, :]
        )
        mixed[h] = jnp.where(lane_half == h % 2, branch, branch_lse)

    def local_heads(start, stop):
        def body(h, _):
            arrived(h + 1)
            local(h)
            return _

        lax.fori_loop(start, stop, body, 0)

    def mix(h):
        l_at = HEAD_DIM - h % 2 * HEAD_DIM
        rows = slice(h * ROWS, (h + 1) * ROWS)
        row = iota((ROWS, 1), 0)
        own, mid, top = mixed[h, rows, :], mid_res[h], top_res[h]
        top = jnp.where(row == 0, top[0:1], top[1:2])
        lse1 = own[:, l_at : l_at + 1]
        lse2 = mid[:, l_at : l_at + 1]
        lse3 = jnp.where(row % 16 == 0, top[:, l_at : l_at + 1], masked_score)
        largest = jnp.maximum(jnp.maximum(lse1, lse2), lse3)
        f1, f2, f3 = jnp.exp(lse1 - largest), jnp.exp(lse2 - largest), jnp.exp(lse3 - largest)
        mixed[h, rows, :] = (f1 * own + f2 * mid + f3 * top) / (f1 + f2 + f3)

    row, col = iota((TOK, TOK), 0), iota((TOK, TOK), 1)
    back = one_hot(row == 8 * (col % ROWS) + col // ROWS)

    def restore(p):
        rows = jnp.where(low, mixed[2 * p], mixed[2 * p + 1]).astype(BF)
        out_ref[:, p * 128 : (p + 1) * 128] = nn_dot(back, rows).astype(BF)

    all_tz = send(topkv.at[0, 0:15], topkv.at[0, 0:15], s_tz, r_tz, sibling)
    two = (z == 0) & (x > 0)
    start = (z <= 2).astype(jnp.int32) + two.astype(jnp.int32)
    late = z > 3
    before = 5 - late.astype(jnp.int32)

    @pl.when(z <= 2)
    def _():
        whole.wait_recv()
        arrived(0)
        local(0)

    @pl.when(two)
    def _():
        arrived(1)
        local(1)

    all_tz.wait_recv()
    for device in x_to:
        send(topkv.at[x], topkv.at[x], s_tx, r_tx, device).start()

    all_mz = send(mkv.at[0, 0:14], mkv.at[0, 0:14], s_mz, r_mz, sibling)
    all_mz.wait_recv()
    share = send(mkv.at[core], mkv.at[core], s_mf, r_mf, sibling)
    share.start()
    share.wait_recv()
    all_qz = send(qmid.at[0:7], qmid.at[0:7], s_qz, r_qz, sibling)
    all_qz.wait_recv()
    v_low = z % 2
    mid_q = qmid[...].reshape(TOK, 128)
    r, n = iota((TOK, 1), 0), iota((1, SPARSE), 1)
    mid_ids_q = slides(block + ((r // ROWS) * 4 + side * 2 + core) * TOK + 8 * (r % ROWS) + z)
    slot = n // ROWS
    device = slot % 16 // 2 * 4 + slot % 2 * 2 + slot // 16
    mid_ids_k = slides(block + device * TOK + 8 * (n % ROWS) + z)
    branch, branch_lse = attend(mid_q, [mkv[...].reshape(SPARSE, 128)], mid_ids_q, mid_ids_k)
    holds = iota((TOK, 128), 1) // HEAD_DIM == v_low
    mid_out[...] = jnp.where(holds, branch, branch_lse).reshape(8, ROWS, 128)
    for zz in z_to:
        send(mid_out.at[zz], mid_res.at[z], s_mr, r_mr, at_z(zz, core)).start()
    mid_res[z] = mid_out[z]

    @pl.when(z > 2)
    def _():
        whole.wait_recv()

    arrived(start)
    local_heads(start, start + 1)

    row, col = iota((64, TOK), 0), iota((64, TOK), 1)
    pick = (row % 8 < 2) & (col == row // 8 * ROWS + row % 8 * 16)
    top_q = nn_dot(one_hot(pick), mid_q).astype(BF)
    r, n = iota((64, 1), 0), iota((1, SPARSE), 1)
    top_ids_q = slides(block + ((r // 8) * 4 + side * 2 + core) * TOK + (r % 8) * 128 + z)
    far_y = n // 2 % 8
    device = (n // 256 * 4 + far_y % 4) * 32 + n // 32 % 8 * 4 + far_y // 4 * 2 + n // 16 % 2
    top_ids_k = slides(device * TOK + n % 2 * 128 + z)
    all_tx = send(topkv.at[0:3], topkv.at[0:3], s_tx, r_tx, sibling)
    all_tx.wait_recv()
    branch, branch_lse = attend(top_q, [topkv[...].reshape(SPARSE, 128)], top_ids_q, top_ids_k)
    holds = iota((64, 128), 1) // HEAD_DIM == v_low
    top_out[...] = jnp.where(holds, branch, branch_lse).reshape(8, 8, 128)
    for zz in z_to:
        send(top_out.at[zz], top_res.at[z], s_tr, r_tr, at_z(zz, core)).start()
    top_res[z] = top_out[z]

    local_heads(start + 1, before)
    local(before)
    all_mr = send(mid_out.at[0:7], mid_res.at[0:7], s_mr, r_mr, sibling)
    all_mr.wait_recv()
    all_tr = send(top_out.at[0:7], top_res.at[0:7], s_tr, r_tr, sibling)
    all_tr.wait_recv()
    for h in range(4):
        mix(h)
    restore(0)
    restore(1)

    @pl.when(late)
    def _():
        arrived(5)
        local(5)

    arrived(6)
    mix(4)
    mix(5)
    restore(2)
    arrived(7)
    local(6)
    mix(6)
    local(7)
    mix(7)
    restore(3)

    whole.wait_send()
    send(kv.at[0, 0], kv.at[2, 0], s_yd, r_yd, partner).wait_send()
    for h in range(HEADS):
        send(kv.at[0, h, 0:7], kv.at[2, h, 0:7], s_y.at[h], r_y.at[h], partner).wait_send()
        forward(h).wait_send()
    all_mz.wait_send()
    share.wait_send()
    all_qz.wait_send()
    all_ty.wait_send()
    all_tz.wait_send()
    all_tx.wait_send()
    all_mr.wait_send()
    all_tr.wait_send()


def shards(queries, keys, values, out_weight, slide_lengths):
    args = (queries, keys, values, slide_lengths)
    dma = pltpu.SemaphoreType.DMA
    width = HEADS * HEAD_DIM
    attention = pl.pallas_call(
        kernel,
        out_shape=jax.ShapeDtypeStruct((TOK, width), BF),
        in_specs=[pl.BlockSpec(memory_space=pltpu.HBM)] * 4,
        out_specs=pl.BlockSpec(memory_space=pltpu.VMEM),
        scratch_shapes=[
            pltpu.VMEM((TOK, width), BF),
            pltpu.VMEM((TOK, width), BF),
            pltpu.VMEM((TOK, width), BF),
            pltpu.SMEM((SLIDES,), jnp.int32),
            pltpu.VMEM((4, HEADS, 8, ROWS, 128), BF),
            pltpu.VMEM((HEADS, 8, ROWS, 128), BF),
            pltpu.VMEM((2, 16, ROWS, 128), BF),
            pltpu.VMEM((8, ROWS, 128), BF),
            pltpu.VMEM((16, 128), BF),
            pltpu.VMEM((8, 16, 128), BF),
            pltpu.VMEM((8, 16, 128), BF),
            pltpu.VMEM((4, 16, 16, 128), BF),
            pltpu.VMEM((8, ROWS, 128), F32),
            pltpu.VMEM((8, 8, 128), F32),
            pltpu.VMEM((8, ROWS, 128), F32),
            pltpu.VMEM((8, 8, 128), F32),
            pltpu.VMEM((HEADS, TOK, 128), F32),
            pltpu.VMEM((TOK, 128), jnp.int32),
            pltpu.VMEM((8, SPARSE), jnp.int32),
            pltpu.VMEM((2, 16, width), BF),
            pltpu.VMEM((2, 16, width), BF),
            pltpu.SemaphoreType.REGULAR, dma((8,)), dma, dma, dma, dma, dma((8,)), dma((8,)), dma((8,)), dma((8,)),
            dma, dma, dma, dma, dma, dma, dma, dma, dma, dma, dma, dma, dma, dma, dma, dma,
        ],
        compiler_params=pltpu.CompilerParams(
            collective_id=0, has_side_effects=True, vmem_limit_bytes=48 * 1024 * 1024
        ),
        name="dilated",
    )(*[pltpu.with_memory_space_constraint(a, pltpu.HBM) for a in args])
    return jnp.dot(attention, out_weight, preferred_element_type=F32).astype(BF)


def solution(mesh):
    rows = P(("outer", "inner"), None)
    return jax.shard_map(
        shards, mesh=mesh, in_specs=(rows, rows, rows, P(), P()), out_specs=rows, check_vma=False
    )
```
